256 devices in a mesh: rep: 8 (over x_lo, y), ep: 32 (over x_hi, z, core).
Axes of the slice: x: 4 (x_hi: 2, x_lo: 2; x = x_hi * 2 + x_lo), y: 4, z: 8, core: 2. Of those that a mesh axis runs over, the one named last changes fastest.
Arguments:
- hidden: bfloat16 [4, 8192, 2, 2048], P(None, ('rep', 'ep')), may hold values from -6 to 6
- out_grad: bfloat16 [4, 8192, 7168], P(None, ('rep', 'ep')), may hold values from -0.5 to 0.5
- route_weight: float32 [4, 8192, 2], P(None, ('rep', 'ep')), may hold values from 0.05 to 1
- expert_ids: int32 [4, 8192, 2], P(None, ('rep', 'ep')), may hold values from 0 to 31, as said below
Outputs:
- grad_down: bfloat16 [32, 2048, 7168], P('ep', None, 'rep')
- expert_load: float32 [32], replicated
The draws below stay inside these ranges and needn't reach their ends.
Inputs may be any that keep to these rules, and one draw needn't show every extreme that they name: `expert_ids`: in each micro-batch the 32 tokens of one device (aligned blocks of 32 tokens) name no expert in more than 4 pairs, and some expert is named in exactly 4; the 2 experts of a token differ.
All inputs are finite; a program needn't handle non-finite values.
Results may differ from the reference program's by a relative error of at most 0.0049.
Values may be sent and summed in bfloat16 or wider, within the bound.
No kernel may reach another device: no remote copies, remote signals or barrier semaphores. Data moves between devices by JAX's collectives and lax.ppermute only.
A program may use at most 192 MiB of HBM per device.

```python
import math
import jax
import jax.numpy as jnp
from jax import lax

D = 7168
FF = 2048
TOK_DEV = 32
MICRO = 4
TOPK = 2
SPECIALIST_COUNT = 32
TOKENS = 8192
CAP = 4
N_REP = 8
N_EP = 32


def dispatched_specialist_group(group_seed_value, position_affinity_boost, position_specialist_pick):
    slot_total = SPECIALIST_COUNT * CAP
    noise_key, forced_key, order_key, turn_key = jax.random.split(group_seed_value, 4)
    gaussian_perturbation = jax.random.randint(noise_key, (slot_total,), 0, 65536, dtype=jnp.int32)
    mandated_specialists = jax.random.randint(forced_key, (), 0, SPECIALIST_COUNT, dtype=jnp.int32)
    plain_affinity = jnp.where(position_specialist_pick == mandated_specialists, jnp.int32(262144), position_affinity_boost + gaussian_perturbation)
    score = plain_affinity * slot_total + jnp.arange(slot_total, dtype=jnp.int32)
    chosen = lax.top_k(score, TOK_DEV * TOPK)[1].astype(jnp.int32)
    ordered = jnp.sort(chosen)
    experts = (ordered // CAP).reshape(TOPK, TOK_DEV).T
    token_order = jax.random.permutation(order_key, TOK_DEV).astype(jnp.int32)
    experts = experts[token_order]
    turn = jax.random.randint(turn_key, (TOK_DEV,), 0, TOPK, dtype=jnp.int32)
    column = (jnp.arange(TOPK, dtype=jnp.int32)[None, :] + turn[:, None]) % TOPK
    return jnp.take_along_axis(experts, column, axis=1).astype(jnp.int32)


def draw_expert_ids(key, part):
    rank_key, group_seed_value = jax.random.split(jax.random.fold_in(key, 7101))
    specialist_ordering = jax.random.permutation(rank_key, SPECIALIST_COUNT).astype(jnp.int32)
    affinity_boost = specialist_ordering * 49152 // SPECIALIST_COUNT
    position_specialist_pick = jnp.arange(SPECIALIST_COUNT * CAP, dtype=jnp.int32) // CAP
    position_affinity_boost = affinity_boost[position_specialist_pick]
    block_total = MICRO * (TOKENS // TOK_DEV)
    group_seed_values = jax.random.split(group_seed_value, block_total)
    dispatched_specialists = jax.vmap(lambda lone_specialist: dispatched_specialist_group(lone_specialist, position_affinity_boost, position_specialist_pick))(group_seed_values)
    return dispatched_specialists.reshape(MICRO, TOKENS, TOPK).astype(jnp.int32)


def strengthened(drawn, own_key, source, target, parts, factor):
    owner, partner = [(jnp.arange(drawn.shape[position]) // (drawn.shape[position] // parts)).reshape([-1 if axis == position else 1 for axis in range(drawn.ndim)]) for position in (source, target)]
    chosen = jax.random.permutation(own_key, parts)[partner]
    strong = (owner == chosen) | (owner == (partner + parts // 2) % parts)
    return jnp.where(strong, factor * drawn, drawn)


def level_of(own_key, shape, cuts, least, top_value):
    def one(dim, blocks):
        steps = jax.random.uniform(jax.random.fold_in(jax.random.fold_in(own_key, 6), dim), (blocks,), jnp.float32, least / len(cuts), top_value / len(cuts))
        return jnp.repeat(jnp.exp(steps), shape[dim] // blocks).reshape((-1,) + (1,) * (len(shape) - dim - 1))

    gain = one(*cuts[0])
    for cut in cuts[1:]:
        gain = gain * one(*cut)
    return gain


def gaussian(key, shape, width, limit, pieces=(), held_as=jnp.bfloat16):
    array = jax.random.normal(key, shape, jnp.float32) * width
    if len(pieces) > 0:
        array = level_of(key, shape, pieces, -0.22, 0.18) * array
    return jnp.clip(array, min=-limit, max=limit).astype(held_as)


def bell_draw_with(own_key, shape, width, limit, cuts, heavy, kind=jnp.bfloat16):
    result = width * jax.random.normal(own_key, shape, jnp.float32)
    if cuts:
        result = result * level_of(own_key, shape, cuts, -0.22, 0.18)
    return jnp.clip(strengthened(result, jax.random.fold_in(own_key, 3), *heavy), -limit, limit).astype(kind)


def setup_inputs(seed: int = 0) -> dict:
    arg_keys = jax.random.split(jax.random.key(seed), 5)
    return {
        "hidden": gaussian(arg_keys[0], (MICRO, TOKENS, TOPK, FF), 1.0, 6.0, ((1, 256),)),
        "out_grad": bell_draw_with(arg_keys[1], (MICRO, TOKENS, D), ((MICRO * TOK_DEV * TOPK * N_REP) ** -0.5), 0.5, ((1, 256),), (1, 2, 256, 6.0)),
        "route_weight": jnp.clip(jnp.exp(math.log(1.0) - 2.9957323 * jax.random.uniform(arg_keys[2], (MICRO, TOKENS, TOPK), jnp.float32) ** level_of(arg_keys[2], (MICRO, TOKENS, TOPK), ((1, 256),), -0.2, 0.2)), 0.05, 1.0),
        "expert_ids": draw_expert_ids(jax.random.fold_in(arg_keys[4], 71), 0),
    }


def reference(hidden, out_grad, route_weight, expert_ids):
    scaled = (route_weight[:, :, :, None] * out_grad[:, :, None, :].astype(jnp.float32)).astype(jnp.bfloat16)
    pair_hidden = hidden.reshape(-1, FF)
    pair_grad = scaled.reshape(-1, D)
    flat_routes = expert_ids.reshape(-1)
    largest = MICRO * N_REP * N_EP * CAP

    def one_expert(expert):
        chosen = flat_routes == expert
        picked = jnp.nonzero(chosen, size=largest, fill_value=0)[0]
        usable = jnp.arange(largest) < jnp.sum(chosen.astype(jnp.int32))
        selected = jnp.where(usable[:, None], pair_hidden[picked], jnp.zeros((), hidden.dtype))
        product = lax.dot_general(selected, pair_grad[picked], (((0,), (0,)), ((), ())), preferred_element_type=jnp.float32)
        return product.astype(jnp.bfloat16)

    grad_down = lax.map(one_expert, jnp.arange(SPECIALIST_COUNT, dtype=jnp.int32))
    tallies = jnp.sum((flat_routes[:, None] == jnp.arange(SPECIALIST_COUNT, dtype=jnp.int32)[None, :]).astype(jnp.float32), axis=0)
    expert_load = tallies * (SPECIALIST_COUNT / (MICRO * TOKENS * TOPK))
    return grad_down, expert_load
```

```python
import functools

import jax
import jax.numpy as jnp
from jax import lax
from jax.experimental import pallas as pl
from jax.experimental.pallas import tpu as pltpu
from jax.sharding import Mesh
from jax.sharding import PartitionSpec as P

REP = ("rep_0", "rep_1")
EP = ("ep_0", "ep_1", "ep_2")
REP_EP = REP + EP
LANES = 128
CAP = 4

CHUNKS = (((0, 0), (0, 1)), ((0, 3), (0, 2)), ((1, 0), (1, 1)), ((1, 3), (1, 2)))
AHEAD = ((), ((0, 1), (0, 3)), ((0, 2), (1, 0)), ((1, 1), (1, 3)))


def tn_dot(a, b):
    return lax.dot_general(a, b, (((0,), (0,)), ((), ())), preferred_element_type=jnp.float32)


def pack_columns(out_grad, ids, weight, offsets, micros):
    tokens, width = out_grad.shape
    count = len(offsets)
    cols = width // count
    per_owner = micros * CAP
    block = tokens // micros

    def kernel(x_ref, ids_ref, weight_ref, *outs):
        def column(row):
            return jnp.transpose(jnp.broadcast_to(row, (tokens, tokens)))[:, :LANES]

        rows = [ids_ref[k : k + 1, :].astype(jnp.float32) for k in range(2)]
        here = lax.broadcasted_iota(jnp.int32, (tokens, tokens), 0)
        there = lax.broadcasted_iota(jnp.int32, (tokens, tokens), 1)
        before = (there < here) & (there // block == here // block)
        base = (lax.broadcasted_iota(jnp.int32, (tokens, LANES), 0) // block * CAP).astype(jnp.float32)
        lane = lax.broadcasted_iota(jnp.int32, (tokens, LANES), 1)
        meta = jnp.zeros((tokens, LANES), jnp.float32)
        for k in range(2):
            mine = column(rows[k])
            hits = jnp.where(before & (rows[0] == mine), 1.0, 0.0) + jnp.where(before & (rows[1] == mine), 1.0, 0.0)
            sub = jnp.sum(hits, axis=1, keepdims=True) + base
            value = column(weight_ref[k : k + 1, :])
            high = value.astype(jnp.bfloat16).astype(jnp.float32)
            middle = (value - high).astype(jnp.bfloat16).astype(jnp.float32)
            low = value - high - middle
            for at, item in ((2 * k, mine), (2 * k + 1, sub), (4 + 3 * k, high), (5 + 3 * k, middle), (6 + 3 * k, low)):
                meta = jnp.where(lane == at, item, meta)
        packed = meta.astype(jnp.bfloat16)
        me_x, me_y = lax.axis_index("rep_0"), lax.axis_index("rep_1")
        nx, ny = 2, 4
        for j, (a, b) in enumerate(offsets):
            at = lax.rem(me_x + a, nx) * ny + lax.rem(me_y + b, ny)
            start = pl.multiple_of(at * cols, LANES)
            outs[j][:, :cols] = x_ref[:, pl.ds(start, cols)]
            outs[j][:, cols:] = packed

    return pl.pallas_call(
        kernel,
        out_shape=[jax.ShapeDtypeStruct((tokens, cols + LANES), jnp.bfloat16)] * count,
        compiler_params=pltpu.CompilerParams(vmem_limit_bytes=24 * 1024 * 1024),
        cost_estimate=pl.CostEstimate(flops=1 << 29, bytes_accessed=4 * 1024 * 1024, transcendentals=0),
        name="pack_columns",
    )(out_grad, ids, weight)


def place_hidden(ids, hidden, owners, micros):
    pairs, width = hidden.shape
    per_owner = micros * CAP
    steps = 4
    here = owners // steps
    block = pairs // micros

    def kernel(ids_ref, h_ref, out_ref, slot_ref, count_ref):
        @pl.when(pl.program_id(0) == 0)
        def _():
            row = ids_ref[...].astype(jnp.float32)
            mine = jnp.transpose(jnp.broadcast_to(row, (pairs, pairs)))
            mine_at = lax.broadcasted_iota(jnp.int32, (pairs, pairs), 0)
            there = lax.broadcasted_iota(jnp.int32, (pairs, pairs), 1)
            before = (there < mine_at) & (there // block == mine_at // block)
            position = jnp.sum(jnp.where(before & (row == mine), 1.0, 0.0), axis=1, keepdims=True)
            base = (lax.broadcasted_iota(jnp.int32, (pairs, LANES), 0) // block * CAP).astype(jnp.float32)
            slot_ref[...] = mine[:, :LANES] * per_owner + position + base
            lane = lax.broadcasted_iota(jnp.int32, (pairs, LANES), 1).astype(jnp.float32)
            count_ref[...] = jnp.sum(jnp.where(lane == mine[:, :LANES], 1.0, 0.0), axis=0, keepdims=True)

        at = lax.broadcasted_iota(jnp.int32, (pairs, here * per_owner), 1)
        at = (at + pl.program_id(0) * (here * per_owner)).astype(jnp.float32)
        pick = jnp.where(slot_ref[:, : here * per_owner] == at, 1.0, 0.0).astype(jnp.bfloat16)
        rows = tn_dot(pick, h_ref[...]).astype(jnp.bfloat16)
        out_ref[:, :, :width] = rows.reshape(here, per_owner, width)
        first = lax.broadcasted_iota(jnp.int32, (here * per_owner, LANES), 0) % per_owner == 0
        spare = jnp.where(first, count_ref[...], 0.0).astype(jnp.bfloat16)
        out_ref[:, :, width:] = spare.reshape(here, per_owner, LANES)

    return pl.pallas_call(
        kernel,
        out_shape=jax.ShapeDtypeStruct((owners, per_owner, width + LANES), jnp.bfloat16),
        grid=(steps,),
        in_specs=[
            pl.BlockSpec((1, pairs), lambda i: (0, 0)),
            pl.BlockSpec((pairs, width), lambda i: (0, 0)),
        ],
        out_specs=pl.BlockSpec((here, per_owner, width + LANES), lambda i: (i, 0, 0)),
        scratch_shapes=[pltpu.VMEM((pairs, LANES), jnp.float32), pltpu.VMEM((1, LANES), jnp.float32)],
        compiler_params=pltpu.CompilerParams(vmem_limit_bytes=16 * 1024 * 1024),
        cost_estimate=pl.CostEstimate(
            flops=2 * owners * per_owner * pairs * width, bytes_accessed=3 * 1024 * 1024, transcendentals=0
        ),
        name="place_hidden",
    )(ids, hidden)


def place_cotangents(blocks, owners, per_owner):
    count = len(blocks)
    tokens, packed = blocks[0].shape
    cols = packed - LANES
    rows = owners * per_owner

    def kernel(*refs):
        out_ref = refs[count]
        at = lax.broadcasted_iota(jnp.int32, (tokens, rows), 1).astype(jnp.float32)
        for j in range(count):
            x = refs[j][:, :cols]
            meta16 = refs[j][:, cols:]
            meta = meta16.astype(jnp.float32)
            p0 = jnp.where(meta[:, 0:1] * per_owner + meta[:, 1:2] == at, 1.0, 0.0).astype(jnp.bfloat16)
            p1 = jnp.where(meta[:, 2:3] * per_owner + meta[:, 3:4] == at, 1.0, 0.0).astype(jnp.bfloat16)
            m0 = tn_dot(p0, meta16)
            m1 = tn_dot(p1, meta16)
            weight = ((m0[:, 4:5] + m0[:, 5:6]) + m0[:, 6:7]) + ((m1[:, 7:8] + m1[:, 8:9]) + m1[:, 9:10])
            picked = tn_dot(p0 + p1, x)
            out_ref[:, j] = (picked * weight).astype(jnp.bfloat16).reshape(owners, per_owner, cols)

    return pl.pallas_call(
        kernel,
        out_shape=jax.ShapeDtypeStruct((owners, count, per_owner, cols), jnp.bfloat16),
        compiler_params=pltpu.CompilerParams(vmem_limit_bytes=24 * 1024 * 1024),
        cost_estimate=pl.CostEstimate(
            flops=2 * count * rows * tokens * (cols + 2 * LANES), bytes_accessed=4 * 1024 * 1024, transcendentals=0
        ),
        name="place_cotangents",
    )(*blocks)


def product(hiddens, cots, total, loads, last):
    count = len(hiddens)
    rows, wide = hiddens[0].shape
    width = wide - LANES
    owners, _, per_owner, cols = cots.shape
    tile = 256
    first = total is None

    def kernel(*refs):
        h = refs[:count]
        spare = refs[count : 2 * count]
        cot_ref = refs[2 * count]
        rest = refs[2 * count + 1 :]
        if first:
            out_ref, load_ref = rest
        else:
            total_ref, seen_ref, out_ref, load_ref = rest
        acc = None
        for j in range(count):
            part = tn_dot(h[j][...], cot_ref[:, j].reshape(rows, cols))
            acc = part if acc is None else acc + part
        if not first:
            acc = acc + total_ref[...]
        out_ref[...] = acc.astype(out_ref.dtype)

        @pl.when(pl.program_id(0) == 0)
        def _():
            seen = None if first else seen_ref[...]
            for j in range(count):
                part = jnp.sum(spare[j][...].astype(jnp.float32), axis=0, keepdims=True)
                seen = part if seen is None else seen + part
            load_ref[...] = seen

    in_specs = [pl.BlockSpec((rows, tile), lambda m: (0, m))] * count
    in_specs += [pl.BlockSpec((rows, LANES), lambda m: (0, width // LANES))] * count
    in_specs += [pl.BlockSpec((owners, count, per_owner, cols), lambda m: (0, 0, 0, 0))]
    args = list(hiddens) * 2 + [cots]
    if not first:
        in_specs += [pl.BlockSpec((tile, cols), lambda m: (m, 0)), pl.BlockSpec((1, LANES), lambda m: (0, 0))]
        args += [total, loads]
    return pl.pallas_call(
        kernel,
        out_shape=[
            jax.ShapeDtypeStruct((width, cols), jnp.bfloat16 if last else jnp.float32),
            jax.ShapeDtypeStruct((1, LANES), jnp.float32),
        ],
        grid=(width // tile,),
        in_specs=in_specs,
        out_specs=[pl.BlockSpec((tile, cols), lambda m: (m, 0)), pl.BlockSpec((1, LANES), lambda m: (0, 0))],
        compiler_params=pltpu.CompilerParams(
            vmem_limit_bytes=28 * 1024 * 1024, dimension_semantics=("arbitrary",)
        ),
        cost_estimate=pl.CostEstimate(
            flops=2 * count * rows * width * cols, bytes_accessed=20 * 1024 * 1024, transcendentals=0
        ),
        name="product",
    )(*args)


def body(hidden, out_grad, route_weight, expert_ids):
    micros, tokens, choices, width = hidden.shape
    model = out_grad.shape[2]
    nx, ny = lax.axis_size("rep_0"), lax.axis_size("rep_1")
    owners = lax.axis_size(EP)
    all_tokens = micros * tokens
    per_owner = micros * CAP

    offsets = [o for pair in CHUNKS for o in pair]
    ids_row = expert_ids.reshape(1, all_tokens * choices)
    ids_by_choice = jnp.transpose(expert_ids, (2, 0, 1)).reshape(choices, all_tokens)
    weight_by_choice = jnp.transpose(route_weight, (2, 0, 1)).reshape(choices, all_tokens)

    sent_hidden = place_hidden(ids_row, hidden.reshape(all_tokens * choices, width), owners, micros)
    mine = lax.all_to_all(sent_hidden, EP, split_axis=0, concat_axis=0, tiled=True)
    mine = mine.reshape(owners * per_owner, width + LANES)

    packed = pack_columns(out_grad.reshape(all_tokens, model), ids_by_choice, weight_by_choice, offsets, micros)
    came = {}
    for (a, b), block in zip(offsets, packed):
        if (a, b) != (0, 0):
            perm = [
                (x * ny + y, ((x + a) % nx) * ny + (y + b) % ny) for x in range(nx) for y in range(ny)
            ]
            block = lax.ppermute(block, REP, perm)
        came[a, b] = block
    blocks = [came[o] for o in offsets]
    blocks = lax.optimization_barrier(blocks)
    came = dict(zip(offsets, blocks))

    ring = lambda n, d: [(i, (i + d) % n) for i in range(n)]
    held = {(0, 0): mine}
    held[1, 0] = lax.ppermute(mine, "rep_0", ring(nx, 1))
    for a in range(2):
        held[a, 1] = lax.ppermute(held[a, 0], "rep_1", ring(ny, 1))
        held[a, 3] = lax.ppermute(held[a, 0], "rep_1", ring(ny, -1))
    held[0, 2] = lax.ppermute(held[0, 1], "rep_1", ring(ny, 1))
    held[1, 2] = lax.ppermute(held[1, 3], "rep_1", ring(ny, -1))

    total = loads = None
    for n, pair in enumerate(CHUNKS):
        placed = place_cotangents([came[o] for o in pair], owners, per_owner)
        cols = placed.shape[-1]
        placed = placed.reshape(owners, len(pair) * per_owner, cols)
        if n == 0:
            placed, held[0, 0] = lax.optimization_barrier((placed, held[0, 0]))
        else:
            placed, *ahead = lax.optimization_barrier((placed, *[held[o] for o in AHEAD[n]]))
            held.update(zip(AHEAD[n], ahead))
        got = lax.all_to_all(placed, EP, split_axis=0, concat_axis=0, tiled=True)
        got = got.reshape(owners, len(pair), per_owner, cols)
        total, loads = product([held[o] for o in pair], got, total, loads, n == len(CHUNKS) - 1)

    experts = owners
    expert_load = loads[0, :experts] * (experts / float(micros * tokens * nx * ny * owners * choices))
    return total[None], expert_load


def solution(mesh):
    finer = Mesh(mesh.devices.reshape(2, 4, 2, 8, 2), REP_EP)
    placed = (
        P(None, REP_EP, None, None),
        P(None, REP_EP, None),
        P(None, REP_EP, None),
        P(None, REP_EP, None),
    )
    return jax.shard_map(
        body, mesh=finer, in_specs=placed, out_specs=(P(EP, None, REP), P()), check_vma=False
    )
```

```python
import functools

import jax
import jax.numpy as jnp
from jax import lax
from jax.experimental import pallas as pl
from jax.experimental.pallas import tpu as pltpu
from jax.sharding import Mesh
from jax.sharding import PartitionSpec as P

REP = ("rep_0", "rep_1")
EP = ("ep_0", "ep_1", "ep_2")
REP_EP = REP + EP
LANES = 128
CAP = 4

CHUNKS = (((0, 0), (0, 1), (0, 3), (0, 2)), ((1, 0), (1, 1), (1, 3), (1, 2)))
AHEAD = ((), ((0, 1), (0, 3), (0, 2), (1, 0)))


def tn_dot(a, b):
    return lax.dot_general(a, b, (((0,), (0,)), ((), ())), preferred_element_type=jnp.float32)


def pack_columns(out_grad, ids, weight, offsets, micros):
    tokens, width = out_grad.shape
    count = len(offsets)
    cols = width // count
    per_owner = micros * CAP
    block = tokens // micros

    def kernel(x_ref, ids_ref, weight_ref, *outs):
        def column(row):
            return jnp.transpose(jnp.broadcast_to(row, (tokens, tokens)))[:, :LANES]

        rows = [ids_ref[k : k + 1, :].astype(jnp.float32) for k in range(2)]
        here = lax.broadcasted_iota(jnp.int32, (tokens, tokens), 0)
        there = lax.broadcasted_iota(jnp.int32, (tokens, tokens), 1)
        before = (there < here) & (there // block == here // block)
        base = (lax.broadcasted_iota(jnp.int32, (tokens, LANES), 0) // block * CAP).astype(jnp.float32)
        lane = lax.broadcasted_iota(jnp.int32, (tokens, LANES), 1)
        meta = jnp.zeros((tokens, LANES), jnp.float32)
        for k in range(2):
            mine = column(rows[k])
            hits = jnp.where(before & (rows[0] == mine), 1.0, 0.0) + jnp.where(before & (rows[1] == mine), 1.0, 0.0)
            sub = jnp.sum(hits, axis=1, keepdims=True) + base
            value = column(weight_ref[k : k + 1, :])
            high = value.astype(jnp.bfloat16).astype(jnp.float32)
            middle = (value - high).astype(jnp.bfloat16).astype(jnp.float32)
            low = value - high - middle
            for at, item in ((2 * k, mine), (2 * k + 1, sub), (4 + 3 * k, high), (5 + 3 * k, middle), (6 + 3 * k, low)):
                meta = jnp.where(lane == at, item, meta)
        packed = meta.astype(jnp.bfloat16)
        me_x, me_y = lax.axis_index("rep_0"), lax.axis_index("rep_1")
        nx, ny = 2, 4
        for j, (a, b) in enumerate(offsets):
            at = lax.rem(me_x + a, nx) * ny + lax.rem(me_y + b, ny)
            start = pl.multiple_of(at * cols, LANES)
            outs[j][:, :cols] = x_ref[:, pl.ds(start, cols)]
            outs[j][:, cols:] = packed

    return pl.pallas_call(
        kernel,
        out_shape=[jax.ShapeDtypeStruct((tokens, cols + LANES), jnp.bfloat16)] * count,
        compiler_params=pltpu.CompilerParams(vmem_limit_bytes=24 * 1024 * 1024),
        cost_estimate=pl.CostEstimate(flops=1 << 29, bytes_accessed=4 * 1024 * 1024, transcendentals=0),
        name="pack_columns",
    )(out_grad, ids, weight)


def place_hidden(ids, hidden, owners, micros):
    pairs, width = hidden.shape
    per_owner = micros * CAP
    steps = 4
    here = owners // steps
    block = pairs // micros

    def kernel(ids_ref, h_ref, out_ref, slot_ref, count_ref):
        @pl.when(pl.program_id(0) == 0)
        def _():
            row = ids_ref[...].astype(jnp.float32)
            mine = jnp.transpose(jnp.broadcast_to(row, (pairs, pairs)))
            mine_at = lax.broadcasted_iota(jnp.int32, (pairs, pairs), 0)
            there = lax.broadcasted_iota(jnp.int32, (pairs, pairs), 1)
            before = (there < mine_at) & (there // block == mine_at // block)
            position = jnp.sum(jnp.where(before & (row == mine), 1.0, 0.0), axis=1, keepdims=True)
            base = (lax.broadcasted_iota(jnp.int32, (pairs, LANES), 0) // block * CAP).astype(jnp.float32)
            slot_ref[...] = mine[:, :LANES] * per_owner + position + base
            lane = lax.broadcasted_iota(jnp.int32, (pairs, LANES), 1).astype(jnp.float32)
            count_ref[...] = jnp.sum(jnp.where(lane == mine[:, :LANES], 1.0, 0.0), axis=0, keepdims=True)

        at = lax.broadcasted_iota(jnp.int32, (pairs, here * per_owner), 1)
        at = (at + pl.program_id(0) * (here * per_owner)).astype(jnp.float32)
        pick = jnp.where(slot_ref[:, : here * per_owner] == at, 1.0, 0.0).astype(jnp.bfloat16)
        rows = tn_dot(pick, h_ref[...]).astype(jnp.bfloat16)
        out_ref[:, :, :width] = rows.reshape(here, per_owner, width)
        first = lax.broadcasted_iota(jnp.int32, (here * per_owner, LANES), 0) % per_owner == 0
        spare = jnp.where(first, count_ref[...], 0.0).astype(jnp.bfloat16)
        out_ref[:, :, width:] = spare.reshape(here, per_owner, LANES)

    return pl.pallas_call(
        kernel,
        out_shape=jax.ShapeDtypeStruct((owners, per_owner, width + LANES), jnp.bfloat16),
        grid=(steps,),
        in_specs=[
            pl.BlockSpec((1, pairs), lambda i: (0, 0)),
            pl.BlockSpec((pairs, width), lambda i: (0, 0)),
        ],
        out_specs=pl.BlockSpec((here, per_owner, width + LANES), lambda i: (i, 0, 0)),
        scratch_shapes=[pltpu.VMEM((pairs, LANES), jnp.float32), pltpu.VMEM((1, LANES), jnp.float32)],
        compiler_params=pltpu.CompilerParams(vmem_limit_bytes=16 * 1024 * 1024),
        cost_estimate=pl.CostEstimate(
            flops=2 * owners * per_owner * pairs * width, bytes_accessed=3 * 1024 * 1024, transcendentals=0
        ),
        name="place_hidden",
    )(ids, hidden)


def place_cotangents(blocks, owners, per_owner):
    count = len(blocks)
    tokens, packed = blocks[0].shape
    cols = packed - LANES
    rows = owners * per_owner

    def kernel(*refs):
        out_ref = refs[count]
        at = lax.broadcasted_iota(jnp.int32, (tokens, rows), 1).astype(jnp.float32)
        for j in range(count):
            x = refs[j][:, :cols]
            meta16 = refs[j][:, cols:]
            meta = meta16.astype(jnp.float32)
            p0 = jnp.where(meta[:, 0:1] * per_owner + meta[:, 1:2] == at, 1.0, 0.0).astype(jnp.bfloat16)
            p1 = jnp.where(meta[:, 2:3] * per_owner + meta[:, 3:4] == at, 1.0, 0.0).astype(jnp.bfloat16)
            m0 = tn_dot(p0, meta16)
            m1 = tn_dot(p1, meta16)
            weight = ((m0[:, 4:5] + m0[:, 5:6]) + m0[:, 6:7]) + ((m1[:, 7:8] + m1[:, 8:9]) + m1[:, 9:10])
            picked = tn_dot(p0 + p1, x)
            out_ref[:, j] = (picked * weight).astype(jnp.bfloat16).reshape(owners, per_owner, cols)

    return pl.pallas_call(
        kernel,
        out_shape=jax.ShapeDtypeStruct((owners, count, per_owner, cols), jnp.bfloat16),
        compiler_params=pltpu.CompilerParams(vmem_limit_bytes=24 * 1024 * 1024),
        cost_estimate=pl.CostEstimate(
            flops=2 * count * rows * tokens * (cols + 2 * LANES), bytes_accessed=4 * 1024 * 1024, transcendentals=0
        ),
        name="place_cotangents",
    )(*blocks)


def product(hiddens, cots, total, loads, last):
    count = len(hiddens)
    rows, wide = hiddens[0].shape
    width = wide - LANES
    owners, _, per_owner, cols = cots.shape
    tile = 256
    first = total is None

    def kernel(*refs):
        h = refs[:count]
        spare = refs[count : 2 * count]
        cot_ref = refs[2 * count]
        rest = refs[2 * count + 1 :]
        if first:
            out_ref, load_ref = rest
        else:
            total_ref, seen_ref, out_ref, load_ref = rest
        acc = None
        for j in range(count):
            part = tn_dot(h[j][...], cot_ref[:, j].reshape(rows, cols))
            acc = part if acc is None else acc + part
        if not first:
            acc = acc + total_ref[...]
        out_ref[...] = acc.astype(out_ref.dtype)

        @pl.when(pl.program_id(0) == 0)
        def _():
            seen = None if first else seen_ref[...]
            for j in range(count):
                part = jnp.sum(spare[j][...].astype(jnp.float32), axis=0, keepdims=True)
                seen = part if seen is None else seen + part
            load_ref[...] = seen

    in_specs = [pl.BlockSpec((rows, tile), lambda m: (0, m))] * count
    in_specs += [pl.BlockSpec((rows, LANES), lambda m: (0, width // LANES))] * count
    in_specs += [pl.BlockSpec((owners, count, per_owner, cols), lambda m: (0, 0, 0, 0))]
    args = list(hiddens) * 2 + [cots]
    if not first:
        in_specs += [pl.BlockSpec((tile, cols), lambda m: (m, 0)), pl.BlockSpec((1, LANES), lambda m: (0, 0))]
        args += [total, loads]
    return pl.pallas_call(
        kernel,
        out_shape=[
            jax.ShapeDtypeStruct((width, cols), jnp.bfloat16 if last else jnp.float32),
            jax.ShapeDtypeStruct((1, LANES), jnp.float32),
        ],
        grid=(width // tile,),
        in_specs=in_specs,
        out_specs=[pl.BlockSpec((tile, cols), lambda m: (m, 0)), pl.BlockSpec((1, LANES), lambda m: (0, 0))],
        compiler_params=pltpu.CompilerParams(
            vmem_limit_bytes=28 * 1024 * 1024, dimension_semantics=("arbitrary",)
        ),
        cost_estimate=pl.CostEstimate(
            flops=2 * count * rows * width * cols, bytes_accessed=20 * 1024 * 1024, transcendentals=0
        ),
        name="product",
    )(*args)


def body(hidden, out_grad, route_weight, expert_ids):
    micros, tokens, choices, width = hidden.shape
    model = out_grad.shape[2]
    nx, ny = lax.axis_size("rep_0"), lax.axis_size("rep_1")
    owners = lax.axis_size(EP)
    all_tokens = micros * tokens
    per_owner = micros * CAP

    offsets = [o for pair in CHUNKS for o in pair]
    ids_row = expert_ids.reshape(1, all_tokens * choices)
    ids_by_choice = jnp.transpose(expert_ids, (2, 0, 1)).reshape(choices, all_tokens)
    weight_by_choice = jnp.transpose(route_weight, (2, 0, 1)).reshape(choices, all_tokens)

    sent_hidden = place_hidden(ids_row, hidden.reshape(all_tokens * choices, width), owners, micros)
    mine = lax.all_to_all(sent_hidden, EP, split_axis=0, concat_axis=0, tiled=True)
    mine = mine.reshape(owners * per_owner, width + LANES)

    packed = pack_columns(out_grad.reshape(all_tokens, model), ids_by_choice, weight_by_choice, offsets, micros)
    came = {}
    for (a, b), block in zip(offsets, packed):
        if (a, b) != (0, 0):
            perm = [
                (x * ny + y, ((x + a) % nx) * ny + (y + b) % ny) for x in range(nx) for y in range(ny)
            ]
            block = lax.ppermute(block, REP, perm)
        came[a, b] = block
    blocks = [came[o] for o in offsets]
    blocks = lax.optimization_barrier(blocks)
    came = dict(zip(offsets, blocks))

    ring = lambda n, d: [(i, (i + d) % n) for i in range(n)]
    held = {(0, 0): mine}
    held[1, 0] = lax.ppermute(mine, "rep_0", ring(nx, 1))
    for a in range(2):
        held[a, 1] = lax.ppermute(held[a, 0], "rep_1", ring(ny, 1))
        held[a, 3] = lax.ppermute(held[a, 0], "rep_1", ring(ny, -1))
    held[0, 2] = lax.ppermute(held[0, 1], "rep_1", ring(ny, 1))
    held[1, 2] = lax.ppermute(held[1, 3], "rep_1", ring(ny, -1))

    total = loads = None
    for n, pair in enumerate(CHUNKS):
        placed = place_cotangents([came[o] for o in pair], owners, per_owner)
        cols = placed.shape[-1]
        placed = placed.reshape(owners, len(pair) * per_owner, cols)
        if n == 0:
            placed, held[0, 0] = lax.optimization_barrier((placed, held[0, 0]))
        else:
            placed, *ahead = lax.optimization_barrier((placed, *[held[o] for o in AHEAD[n]]))
            held.update(zip(AHEAD[n], ahead))
        got = lax.all_to_all(placed, EP, split_axis=0, concat_axis=0, tiled=True)
        got = got.reshape(owners, len(pair), per_owner, cols)
        total, loads = product([held[o] for o in pair], got, total, loads, n == len(CHUNKS) - 1)

    experts = owners
    expert_load = loads[0, :experts] * (experts / float(micros * tokens * nx * ny * owners * choices))
    return total[None], expert_load


def solution(mesh):
    finer = Mesh(mesh.devices.reshape(2, 4, 2, 8, 2), REP_EP)
    placed = (
        P(None, REP_EP, None, None),
        P(None, REP_EP, None),
        P(None, REP_EP, None),
        P(None, REP_EP, None),
    )
    return jax.shard_map(
        body, mesh=finer, in_specs=placed, out_specs=(P(EP, None, REP), P()), check_vma=False
    )
```

```python
import functools

import jax
import jax.numpy as jnp
from jax import lax
from jax.experimental import pallas as pl
from jax.experimental.pallas import tpu as pltpu
from jax.sharding import Mesh
from jax.sharding import PartitionSpec as P

REP = ("rep_0", "rep_1")
EP = ("ep_0", "ep_1", "ep_2")
REP_EP = REP + EP
LANES = 128
CAP = 4

CHUNKS = (((0, 0), (0, 1), (0, 3), (0, 2)), ((1, 0), (1, 1), (1, 3), (1, 2)))


def tn_dot(a, b):
    return lax.dot_general(a, b, (((0,), (0,)), ((), ())), preferred_element_type=jnp.float32)


def pack_columns(out_grad, ids, weight, offsets, micros):
    tokens, width = out_grad.shape
    count = len(offsets)
    cols = width // count
    per_owner = micros * CAP
    block = tokens // micros

    def kernel(x_ref, ids_ref, weight_ref, *outs):
        def column(row):
            return jnp.transpose(jnp.broadcast_to(row, (tokens, tokens)))[:, :LANES]

        rows = [ids_ref[k : k + 1, :].astype(jnp.float32) for k in range(2)]
        here = lax.broadcasted_iota(jnp.int32, (tokens, tokens), 0)
        there = lax.broadcasted_iota(jnp.int32, (tokens, tokens), 1)
        before = (there < here) & (there // block == here // block)
        base = (lax.broadcasted_iota(jnp.int32, (tokens, LANES), 0) // block * CAP).astype(jnp.float32)
        lane = lax.broadcasted_iota(jnp.int32, (tokens, LANES), 1)
        meta = jnp.zeros((tokens, LANES), jnp.float32)
        for k in range(2):
            mine = column(rows[k])
            hits = jnp.where(before & (rows[0] == mine), 1.0, 0.0) + jnp.where(before & (rows[1] == mine), 1.0, 0.0)
            sub = jnp.sum(hits, axis=1, keepdims=True) + base
            value = column(weight_ref[k : k + 1, :])
            high = value.astype(jnp.bfloat16).astype(jnp.float32)
            middle = (value - high).astype(jnp.bfloat16).astype(jnp.float32)
            low = value - high - middle
            for at, item in ((2 * k, mine), (2 * k + 1, sub), (4 + 3 * k, high), (5 + 3 * k, middle), (6 + 3 * k, low)):
                meta = jnp.where(lane == at, item, meta)
        packed = meta.astype(jnp.bfloat16)
        me_x, me_y = lax.axis_index("rep_0"), lax.axis_index("rep_1")
        nx, ny = 2, 4
        for j, (a, b) in enumerate(offsets):
            at = lax.rem(me_x + a, nx) * ny + lax.rem(me_y + b, ny)
            start = pl.multiple_of(at * cols, LANES)
            outs[j][:, :cols] = x_ref[:, pl.ds(start, cols)]
            outs[j][:, cols:] = packed

    return pl.pallas_call(
        kernel,
        out_shape=[jax.ShapeDtypeStruct((tokens, cols + LANES), jnp.bfloat16)] * count,
        compiler_params=pltpu.CompilerParams(vmem_limit_bytes=24 * 1024 * 1024),
        cost_estimate=pl.CostEstimate(flops=1 << 29, bytes_accessed=4 * 1024 * 1024, transcendentals=0),
        name="pack_columns",
    )(out_grad, ids, weight)


def place_hidden(ids, hidden, owners, micros):
    pairs, width = hidden.shape
    per_owner = micros * CAP
    steps = 4
    here = owners // steps
    block = pairs // micros

    def kernel(ids_ref, h_ref, out_ref, slot_ref, count_ref):
        @pl.when(pl.program_id(0) == 0)
        def _():
            row = ids_ref[...].astype(jnp.float32)
            mine = jnp.transpose(jnp.broadcast_to(row, (pairs, pairs)))
            mine_at = lax.broadcasted_iota(jnp.int32, (pairs, pairs), 0)
            there = lax.broadcasted_iota(jnp.int32, (pairs, pairs), 1)
            before = (there < mine_at) & (there // block == mine_at // block)
            position = jnp.sum(jnp.where(before & (row == mine), 1.0, 0.0), axis=1, keepdims=True)
            base = (lax.broadcasted_iota(jnp.int32, (pairs, LANES), 0) // block * CAP).astype(jnp.float32)
            slot_ref[...] = mine[:, :LANES] * per_owner + position + base
            lane = lax.broadcasted_iota(jnp.int32, (pairs, LANES), 1).astype(jnp.float32)
            count_ref[...] = jnp.sum(jnp.where(lane == mine[:, :LANES], 1.0, 0.0), axis=0, keepdims=True)

        at = lax.broadcasted_iota(jnp.int32, (pairs, here * per_owner), 1)
        at = (at + pl.program_id(0) * (here * per_owner)).astype(jnp.float32)
        pick = jnp.where(slot_ref[:, : here * per_owner] == at, 1.0, 0.0).astype(jnp.bfloat16)
        rows = tn_dot(pick, h_ref[...]).astype(jnp.bfloat16)
        out_ref[:, :, :width] = rows.reshape(here, per_owner, width)
        first = lax.broadcasted_iota(jnp.int32, (here * per_owner, LANES), 0) % per_owner == 0
        spare = jnp.where(first, count_ref[...], 0.0).astype(jnp.bfloat16)
        out_ref[:, :, width:] = spare.reshape(here, per_owner, LANES)

    return pl.pallas_call(
        kernel,
        out_shape=jax.ShapeDtypeStruct((owners, per_owner, width + LANES), jnp.bfloat16),
        grid=(steps,),
        in_specs=[
            pl.BlockSpec((1, pairs), lambda i: (0, 0)),
            pl.BlockSpec((pairs, width), lambda i: (0, 0)),
        ],
        out_specs=pl.BlockSpec((here, per_owner, width + LANES), lambda i: (i, 0, 0)),
        scratch_shapes=[pltpu.VMEM((pairs, LANES), jnp.float32), pltpu.VMEM((1, LANES), jnp.float32)],
        compiler_params=pltpu.CompilerParams(vmem_limit_bytes=16 * 1024 * 1024),
        cost_estimate=pl.CostEstimate(
            flops=2 * owners * per_owner * pairs * width, bytes_accessed=3 * 1024 * 1024, transcendentals=0
        ),
        name="place_hidden",
    )(ids, hidden)


def place_cotangents(blocks, owners, per_owner):
    count = len(blocks)
    tokens, packed = blocks[0].shape
    cols = packed - LANES
    rows = owners * per_owner

    def kernel(*refs):
        out_ref = refs[count]
        at = lax.broadcasted_iota(jnp.int32, (tokens, rows), 1).astype(jnp.float32)
        for j in range(count):
            x = refs[j][:, :cols]
            meta16 = refs[j][:, cols:]
            meta = meta16.astype(jnp.float32)
            p0 = jnp.where(meta[:, 0:1] * per_owner + meta[:, 1:2] == at, 1.0, 0.0).astype(jnp.bfloat16)
            p1 = jnp.where(meta[:, 2:3] * per_owner + meta[:, 3:4] == at, 1.0, 0.0).astype(jnp.bfloat16)
            m0 = tn_dot(p0, meta16)
            m1 = tn_dot(p1, meta16)
            weight = ((m0[:, 4:5] + m0[:, 5:6]) + m0[:, 6:7]) + ((m1[:, 7:8] + m1[:, 8:9]) + m1[:, 9:10])
            picked = tn_dot(p0 + p1, x)
            out_ref[:, j] = (picked * weight).astype(jnp.bfloat16).reshape(owners, per_owner, cols)

    return pl.pallas_call(
        kernel,
        out_shape=jax.ShapeDtypeStruct((owners, count, per_owner, cols), jnp.bfloat16),
        compiler_params=pltpu.CompilerParams(vmem_limit_bytes=24 * 1024 * 1024),
        cost_estimate=pl.CostEstimate(
            flops=2 * count * rows * tokens * (cols + 2 * LANES), bytes_accessed=4 * 1024 * 1024, transcendentals=0
        ),
        name="place_cotangents",
    )(*blocks)


def product(pieces, cots, total, loads, last):
    count = len(pieces)
    wide = pieces[0][0].shape[1]
    width = wide - LANES
    owners, _, per_owner, cols = cots.shape
    tile = 512
    first = total is None

    def kernel(*refs):
        h = refs[:count]
        spare = refs[count : 2 * count]
        cot_ref = refs[2 * count]
        rest = refs[2 * count + 1 :]
        if first:
            out_ref, load_ref = rest
        else:
            total_ref, seen_ref, out_ref, load_ref = rest
        acc = None
        for n, (piece, block, start) in enumerate(pieces):
            rows = piece.shape[0]
            at = start // per_owner
            part = tn_dot(h[n][...], cot_ref[at : at + rows // per_owner, block].reshape(rows, cols))
            acc = part if acc is None else acc + part
        if not first:
            acc = acc + total_ref[...]
        out_ref[...] = acc.astype(out_ref.dtype)

        @pl.when(pl.program_id(0) == 0)
        def _():
            seen = None if first else seen_ref[...]
            for n in range(count):
                part = jnp.sum(spare[n][...].astype(jnp.float32), axis=0, keepdims=True)
                seen = part if seen is None else seen + part
            load_ref[...] = seen

    in_specs = [pl.BlockSpec((p.shape[0], tile), lambda m: (0, m)) for p, _, _ in pieces]
    in_specs += [pl.BlockSpec((p.shape[0], LANES), lambda m: (0, width // LANES)) for p, _, _ in pieces]
    in_specs += [pl.BlockSpec(cots.shape, lambda m: (0, 0, 0, 0))]
    args = [p for p, _, _ in pieces] * 2 + [cots]
    if not first:
        in_specs += [pl.BlockSpec((tile, cols), lambda m: (m, 0)), pl.BlockSpec((1, LANES), lambda m: (0, 0))]
        args += [total, loads]
    rows = sum(p.shape[0] for p, _, _ in pieces)
    return pl.pallas_call(
        kernel,
        out_shape=[
            jax.ShapeDtypeStruct((width, cols), jnp.bfloat16 if last else jnp.float32),
            jax.ShapeDtypeStruct((1, LANES), jnp.float32),
        ],
        grid=(width // tile,),
        in_specs=in_specs,
        out_specs=[pl.BlockSpec((tile, cols), lambda m: (m, 0)), pl.BlockSpec((1, LANES), lambda m: (0, 0))],
        compiler_params=pltpu.CompilerParams(
            vmem_limit_bytes=63 * 1024 * 1024, dimension_semantics=("arbitrary",)
        ),
        cost_estimate=pl.CostEstimate(
            flops=2 * rows * width * cols, bytes_accessed=20 * 1024 * 1024, transcendentals=0
        ),
        name="product",
    )(*args)


def body(hidden, out_grad, route_weight, expert_ids):
    micros, tokens, choices, width = hidden.shape
    model = out_grad.shape[2]
    nx, ny = lax.axis_size("rep_0"), lax.axis_size("rep_1")
    owners = lax.axis_size(EP)
    all_tokens = micros * tokens
    per_owner = micros * CAP

    offsets = [o for pair in CHUNKS for o in pair]
    ids_row = expert_ids.reshape(1, all_tokens * choices)
    ids_by_choice = jnp.transpose(expert_ids, (2, 0, 1)).reshape(choices, all_tokens)
    weight_by_choice = jnp.transpose(route_weight, (2, 0, 1)).reshape(choices, all_tokens)

    sent_hidden = place_hidden(ids_row, hidden.reshape(all_tokens * choices, width), owners, micros)
    mine = lax.all_to_all(sent_hidden, EP, split_axis=0, concat_axis=0, tiled=True)
    mine = mine.reshape(owners * per_owner, width + LANES)

    packed = pack_columns(out_grad.reshape(all_tokens, model), ids_by_choice, weight_by_choice, offsets, micros)
    came = {}
    for (a, b), block in zip(offsets, packed):
        if (a, b) != (0, 0):
            perm = [
                (x * ny + y, ((x + a) % nx) * ny + (y + b) % ny) for x in range(nx) for y in range(ny)
            ]
            block = lax.ppermute(block, REP, perm)
        came[a, b] = block
    blocks = [came[o] for o in offsets]
    blocks = lax.optimization_barrier(blocks)
    came = dict(zip(offsets, blocks))

    ring = lambda n, d: [(i, (i + d) % n) for i in range(n)]
    half = owners * per_owner // 2

    def gathered(block):
        up = lax.ppermute(block, "rep_1", ring(ny, 1))
        down = lax.ppermute(block, "rep_1", ring(ny, -1))
        top = lax.ppermute(up[:half], "rep_1", ring(ny, 1))
        bottom = lax.ppermute(down[half:], "rep_1", ring(ny, -1))
        return [block, up, down, top, bottom]

    total = loads = None
    held = other = None
    for n, pair in enumerate(CHUNKS):
        placed = place_cotangents([came[o] for o in pair], owners, per_owner)
        cols = placed.shape[-1]
        placed = placed.reshape(owners, len(pair) * per_owner, cols)
        if n == 0:
            placed, mine = lax.optimization_barrier((placed, mine))
            other = lax.ppermute(mine, "rep_0", ring(nx, 1))
            held = gathered(mine)
        else:
            placed, other, *held = lax.optimization_barrier((placed, other, *held))
            ahead = gathered(other)
        got = lax.all_to_all(placed, EP, split_axis=0, concat_axis=0, tiled=True)
        got = got.reshape(owners, len(pair), per_owner, cols)
        block, up, down, top, bottom = held if n == 0 else ahead
        pieces = [(block, 0, 0), (up, 1, 0), (down, 2, 0), (top, 3, 0), (bottom, 3, half)]
        waiting = (pieces, got)
        if n == 0:
            first_waiting = waiting
    block, up, down, top, bottom = held
    pieces = [(block, 0, 0), (up, 1, 0), (down, 2, 0), (top, 3, 0), (bottom, 3, half)]
    total, loads = product(pieces, first_waiting[1], None, None, False)
    total, loads = product(*waiting, total, loads, True)

    experts = owners
    expert_load = loads[0, :experts] * (experts / float(micros * tokens * nx * ny * owners * choices))
    return total[None], expert_load


def solution(mesh):
    finer = Mesh(mesh.devices.reshape(2, 4, 2, 8, 2), REP_EP)
    placed = (
        P(None, REP_EP, None, None),
        P(None, REP_EP, None),
        P(None, REP_EP, None),
        P(None, REP_EP, None),
    )
    return jax.shard_map(
        body, mesh=finer, in_specs=placed, out_specs=(P(EP, None, REP), P()), check_vma=False
    )
```

```python
import functools

import jax
import jax.numpy as jnp
from jax import lax
from jax.experimental import pallas as pl
from jax.experimental.pallas import tpu as pltpu
from jax.sharding import Mesh
from jax.sharding import PartitionSpec as P

REP = ("rep_0", "rep_1")
EP = ("ep_0", "ep_1", "ep_2")
REP_EP = REP + EP
LANES = 128
CAP = 4
META = 16
BLOCKS = 4
RELATIVE = ((0, 0), (0, 1), (1, 0), (1, 1))

CHUNKS = (((0, 0), (0, 1), (0, 3), (0, 2)), ((1, 0), (1, 1), (1, 3), (1, 2)))


def tn_dot(a, b):
    return lax.dot_general(a, b, (((0,), (0,)), ((), ())), preferred_element_type=jnp.float32)


def pack_columns(out_grad, ids, weight, offsets, micros):
    tokens, width = out_grad.shape
    count = len(offsets)
    cols = width // count
    block = tokens // micros
    nx, ny = lax.axis_size("rep_0"), lax.axis_size("rep_1")

    def kernel(x_ref, ids_ref, weight_ref, *outs):
        rows = [ids_ref[k : k + 1, :].astype(jnp.float32) for k in range(2)]
        columns = [jnp.transpose(jnp.broadcast_to(row, (tokens, tokens))) for row in rows]
        there = lax.broadcasted_iota(jnp.int32, (tokens, tokens), 0)
        here = lax.broadcasted_iota(jnp.int32, (tokens, tokens), 1)
        before = (there < here) & (there // block == here // block)
        base = (lax.broadcasted_iota(jnp.int32, (1, tokens), 1) // block * CAP).astype(jnp.float32)
        line = lax.broadcasted_iota(jnp.int32, (META, tokens), 0)
        meta = jnp.zeros((META, tokens), jnp.float32)
        for k in range(2):
            hits = jnp.where(before & (columns[0] == rows[k]), 1.0, 0.0)
            hits = hits + jnp.where(before & (columns[1] == rows[k]), 1.0, 0.0)
            sub = jnp.sum(hits, axis=0, keepdims=True) + base
            value = weight_ref[k : k + 1, :]
            high = value.astype(jnp.bfloat16).astype(jnp.float32)
            middle = (value - high).astype(jnp.bfloat16).astype(jnp.float32)
            low = value - high - middle
            for at, item in enumerate((rows[k], sub, high, middle, low)):
                meta = jnp.where(line == 5 * k + at, item, meta)
        packed = meta.astype(jnp.bfloat16)
        me_x, me_y = lax.axis_index("rep_0"), lax.axis_index("rep_1")
        for j, (a, b) in enumerate(offsets):
            at = lax.rem(me_x + a, nx) * ny + lax.rem(me_y + b, ny)
            start = pl.multiple_of(at * cols, LANES)
            outs[j][:tokens, :] = x_ref[:, pl.ds(start, cols)]
            outs[j][tokens:, :tokens] = packed
            outs[j][tokens:, tokens:] = jnp.zeros((META, cols - tokens), jnp.bfloat16)

    return pl.pallas_call(
        kernel,
        out_shape=[jax.ShapeDtypeStruct((tokens + META, cols), jnp.bfloat16)] * count,
        compiler_params=pltpu.CompilerParams(vmem_limit_bytes=24 * 1024 * 1024),
        cost_estimate=pl.CostEstimate(flops=1 << 29, bytes_accessed=4 * 1024 * 1024, transcendentals=0),
        name="pack_columns",
    )(out_grad, ids, weight)


def assemble(blocks):
    count = len(blocks)
    rows, cols = blocks[0].shape
    tokens = rows - META

    def kernel(*refs):
        out_ref = refs[count]
        for j in range(count):
            out_ref[j * tokens : (j + 1) * tokens, :] = refs[j][:tokens, :]
            out_ref[count * tokens :, j * tokens : (j + 1) * tokens] = refs[j][tokens:, :tokens]
        out_ref[count * tokens :, count * tokens :] = jnp.zeros((META, cols - count * tokens), jnp.bfloat16)

    return pl.pallas_call(
        kernel,
        out_shape=jax.ShapeDtypeStruct((count * tokens + META, cols), jnp.bfloat16),
        compiler_params=pltpu.CompilerParams(vmem_limit_bytes=16 * 1024 * 1024),
        cost_estimate=pl.CostEstimate(flops=1 << 29, bytes_accessed=2 * 1024 * 1024, transcendentals=0),
        name="assemble",
    )(*blocks)


def place_hidden(ids, hidden, owners, micros):
    pairs, width = hidden.shape
    per_owner = micros * CAP
    steps = 4
    here = owners // steps
    block = pairs // micros

    def kernel(ids_ref, h_ref, out_ref, slot_ref, count_ref):
        @pl.when(pl.program_id(0) == 0)
        def _():
            row = ids_ref[...].astype(jnp.float32)
            mine = jnp.transpose(jnp.broadcast_to(row, (pairs, pairs)))
            mine_at = lax.broadcasted_iota(jnp.int32, (pairs, pairs), 0)
            there = lax.broadcasted_iota(jnp.int32, (pairs, pairs), 1)
            before = (there < mine_at) & (there // block == mine_at // block)
            position = jnp.sum(jnp.where(before & (row == mine), 1.0, 0.0), axis=1, keepdims=True)
            base = (lax.broadcasted_iota(jnp.int32, (pairs, LANES), 0) // block * CAP).astype(jnp.float32)
            slot_ref[...] = mine[:, :LANES] * per_owner + position + base
            lane = lax.broadcasted_iota(jnp.int32, (pairs, LANES), 1).astype(jnp.float32)
            count_ref[...] = jnp.sum(jnp.where(lane == mine[:, :LANES], 1.0, 0.0), axis=0, keepdims=True)

        at = lax.broadcasted_iota(jnp.int32, (pairs, here * per_owner), 1)
        at = (at + pl.program_id(0) * (here * per_owner)).astype(jnp.float32)
        pick = jnp.where(slot_ref[:, : here * per_owner] == at, 1.0, 0.0).astype(jnp.bfloat16)
        rows = tn_dot(pick, h_ref[...]).astype(jnp.bfloat16)
        out_ref[:, :, :width] = rows.reshape(here, per_owner, width)
        first = lax.broadcasted_iota(jnp.int32, (here * per_owner, LANES), 0) % per_owner == 0
        spare = jnp.where(first, count_ref[...], 0.0).astype(jnp.bfloat16)
        out_ref[:, :, width:] = spare.reshape(here, per_owner, LANES)

    return pl.pallas_call(
        kernel,
        out_shape=jax.ShapeDtypeStruct((owners, per_owner, width + LANES), jnp.bfloat16),
        grid=(steps,),
        in_specs=[
            pl.BlockSpec((1, pairs), lambda i: (0, 0)),
            pl.BlockSpec((pairs, width), lambda i: (0, 0)),
        ],
        out_specs=pl.BlockSpec((here, per_owner, width + LANES), lambda i: (i, 0, 0)),
        scratch_shapes=[pltpu.VMEM((pairs, LANES), jnp.float32), pltpu.VMEM((1, LANES), jnp.float32)],
        compiler_params=pltpu.CompilerParams(vmem_limit_bytes=16 * 1024 * 1024),
        cost_estimate=pl.CostEstimate(
            flops=2 * owners * per_owner * pairs * width, bytes_accessed=3 * 1024 * 1024, transcendentals=0
        ),
        name="place_hidden",
    )(ids, hidden)


class Site:
    def __init__(self, sizes):
        self.nx, self.nz, self.nc = sizes
        self.x, self.z, self.c = lax.axis_index("ep_0"), lax.axis_index("ep_1"), lax.axis_index("ep_2")

    def owner(self, rel, dz):
        x = lax.rem(self.x + rel[0], self.nx)
        z = lax.rem(self.z + dz + self.nz, self.nz)
        return (x * self.nz + z) * self.nc + lax.rem(self.c + rel[1], self.nc)


def rows_for(site, ref, block, blocks, tokens, per_owner, dz):
    spot = lax.broadcasted_iota(jnp.int32, (len(RELATIVE) * per_owner, 1), 0)
    want = spot - spot // per_owner * per_owner
    for n, rel in enumerate(RELATIVE):
        want = want + jnp.where(spot // per_owner == n, site.owner(rel, dz) * per_owner, 0)
    want = want.astype(jnp.float32)
    meta = ref[blocks * tokens : blocks * tokens + META, block * tokens : (block + 1) * tokens].astype(jnp.float32)
    weight = jnp.zeros((1, 1), jnp.float32)
    hit = None
    for k in range(2):
        at = 5 * k
        mine = meta[at : at + 1] * per_owner + meta[at + 1 : at + 2] == want
        value = (meta[at + 2 : at + 3] + meta[at + 3 : at + 4]) + meta[at + 4 : at + 5]
        weight = weight + jnp.sum(jnp.where(mine, value, 0.0), axis=1, keepdims=True)
        hit = mine if hit is None else hit | mine
    pick = jnp.where(hit, 1.0, 0.0).astype(jnp.bfloat16)
    x = ref[block * tokens : (block + 1) * tokens, :]
    picked = jnp.dot(pick, x, preferred_element_type=jnp.float32)
    return (picked * weight).astype(jnp.bfloat16)


def stage(name, kernel, inputs, shapes, flops):
    return pl.pallas_call(
        kernel,
        out_shape=[jax.ShapeDtypeStruct(shape, jnp.bfloat16) for shape in shapes],
        compiler_params=pltpu.CompilerParams(vmem_limit_bytes=20 * 1024 * 1024),
        cost_estimate=pl.CostEstimate(flops=flops, bytes_accessed=4 * 1024 * 1024, transcendentals=0),
        name=name,
    )(*inputs)


def put(outs, rows, first, per_owner):
    for n in range(len(RELATIVE)):
        outs[n][first : first + per_owner, :] = rows[n * per_owner : (n + 1) * per_owner]


def place_near(sizes, own, below, above, tokens, per_owner):
    cols = own.shape[1]

    def kernel(own_ref, below_ref, above_ref, *outs):
        site = Site(sizes)
        for m, ref in enumerate((own_ref, below_ref, above_ref)):
            for j in range(BLOCKS):
                rows = rows_for(site, ref, j, BLOCKS, tokens, per_owner, 0)
                put(outs, rows, (m * BLOCKS + j) * per_owner, per_owner)

    shapes = [(3 * BLOCKS * per_owner, cols)] * len(RELATIVE)
    return stage("place_near", kernel, (own, below, above), shapes, 1 << 30)


def place_middle(sizes, below, above, tokens, per_owner):
    cols = below.shape[1]
    part = BLOCKS // 2
    head = part * tokens

    def kernel(below_ref, above_ref, *outs):
        site = Site(sizes)
        outs, going = outs[: len(RELATIVE)], outs[len(RELATIVE) :]
        for m, (ref, dz, kept) in enumerate(((below_ref, 1, 0), (above_ref, -1, part))):
            out = going[m]
            out[:head, :] = ref[kept * tokens : kept * tokens + head, :]
            out[head : head + META, :head] = ref[BLOCKS * tokens :, kept * tokens : kept * tokens + head]
            out[head : head + META, head:] = jnp.zeros((META, cols - head), jnp.bfloat16)
            for j in range(part):
                rows = rows_for(site, ref, part - kept + j, BLOCKS, tokens, per_owner, dz)
                first = head + META + j * len(RELATIVE) * per_owner
                out[first : first + len(RELATIVE) * per_owner, :] = rows
        for m, ref in enumerate((below_ref, above_ref)):
            for j in range(BLOCKS):
                rows = rows_for(site, ref, j, BLOCKS, tokens, per_owner, 0)
                put(outs, rows, (m * BLOCKS + j) * per_owner, per_owner)

    shapes = [(2 * BLOCKS * per_owner, cols)] * len(RELATIVE)
    shapes += [(head + META + part * len(RELATIVE) * per_owner, cols)] * 2
    return stage("place_middle", kernel, (below, above), shapes, 1 << 30)


def place_far(sizes, below, above, tokens, per_owner):
    cols = below.shape[1]
    part = BLOCKS // 2
    head = part * tokens
    wide = len(RELATIVE) * per_owner

    def kernel(below_ref, above_ref, *outs):
        site = Site(sizes)
        outs, going = outs[: len(RELATIVE)], outs[len(RELATIVE) :]
        for m, (ref, dz) in enumerate(((below_ref, 1), (above_ref, -1))):
            for j in range(part):
                going[m][j * wide : (j + 1) * wide, :] = rows_for(site, ref, j, part, tokens, per_owner, dz)
        for m, (ref, kept) in enumerate(((below_ref, 0), (above_ref, part))):
            for j in range(part):
                rows = rows_for(site, ref, j, part, tokens, per_owner, 0)
                put(outs, rows, (m * BLOCKS + kept + j) * per_owner, per_owner)
                first = head + META + j * wide
                put(outs, ref[first : first + wide, :], (m * BLOCKS + part - kept + j) * per_owner, per_owner)

    shapes = [(2 * BLOCKS * per_owner, cols)] * len(RELATIVE) + [(part * wide, cols)] * 2
    return stage("place_far", kernel, (below, above), shapes, 1 << 30)


def place_last(below, above, per_owner):
    cols = below.shape[1]
    part = BLOCKS // 2
    wide = len(RELATIVE) * per_owner

    def kernel(below_ref, above_ref, *outs):
        for m, ref in enumerate((below_ref, above_ref)):
            for j in range(part):
                put(outs, ref[j * wide : (j + 1) * wide, :], (m * part + j) * per_owner, per_owner)

    return stage("place_last", kernel, (below, above), [(BLOCKS * per_owner, cols)] * len(RELATIVE), 1 << 28)


GROUPS = (
    [(dz, j) for dz in (0, -1, 1) for j in range(4)],
    [(dz, j) for dz in (-2, 2) for j in range(4)],
    [(dz, j) for dz in (-3, 3) for j in range(4)],
    [(4, j) for j in range(4)],
)


def product(sizes, pieces, groups, per_owner, total, loads, last):
    count = len(pieces)
    wide = pieces[0][0].shape[1]
    width = wide - LANES
    flat = [x for group in groups for x in group]
    cols = flat[0].shape[1]
    owners = sizes[0] * sizes[1] * sizes[2]
    per_block = owners * per_owner
    tile = 512
    first = total is None

    def kernel(*refs):
        h = refs[:count]
        spare = refs[count : 2 * count]
        sent = refs[2 * count : 2 * count + len(flat)]
        rest = refs[2 * count + len(flat) :]
        if first:
            out_ref, load_ref, cot_ref = rest
        else:
            total_ref, seen_ref, out_ref, load_ref, cot_ref = rest

        @pl.when(pl.program_id(0) == 0)
        def _():
            site = Site(sizes)
            n = 0
            for runs in GROUPS:
                for rel in RELATIVE:
                    for r, (dz, block) in enumerate(runs):
                        at = pl.multiple_of(block * per_block + site.owner(rel, dz) * per_owner, per_owner)
                        cot_ref[pl.ds(at, per_owner), :] = sent[n][r * per_owner : (r + 1) * per_owner, :]
                    n += 1
            seen = None if first else seen_ref[...]
            for n in range(count):
                part = jnp.sum(spare[n][...].astype(jnp.float32), axis=0, keepdims=True)
                seen = part if seen is None else seen + part
            load_ref[...] = seen

        acc = None
        for n, (piece, block, start) in enumerate(pieces):
            at = block * per_block + start
            part = tn_dot(h[n][...], cot_ref[at : at + piece.shape[0], :])
            acc = part if acc is None else acc + part
        if not first:
            acc = acc + total_ref[...]
        out_ref[...] = acc.astype(out_ref.dtype)

    in_specs = [pl.BlockSpec((p.shape[0], tile), lambda m: (0, m)) for p, _, _ in pieces]
    in_specs += [pl.BlockSpec((p.shape[0], LANES), lambda m: (0, width // LANES)) for p, _, _ in pieces]
    in_specs += [pl.BlockSpec(x.shape, lambda m: (0, 0)) for x in flat]
    args = [p for p, _, _ in pieces] * 2 + flat
    if not first:
        in_specs += [pl.BlockSpec((tile, cols), lambda m: (m, 0)), pl.BlockSpec((1, LANES), lambda m: (0, 0))]
        args += [total, loads]
    rows = sum(p.shape[0] for p, _, _ in pieces)
    return pl.pallas_call(
        kernel,
        out_shape=[
            jax.ShapeDtypeStruct((width, cols), jnp.bfloat16 if last else jnp.float32),
            jax.ShapeDtypeStruct((1, LANES), jnp.float32),
        ],
        grid=(width // tile,),
        in_specs=in_specs,
        out_specs=[pl.BlockSpec((tile, cols), lambda m: (m, 0)), pl.BlockSpec((1, LANES), lambda m: (0, 0))],
        scratch_shapes=[pltpu.VMEM((BLOCKS * per_block, cols), jnp.bfloat16)],
        compiler_params=pltpu.CompilerParams(
            vmem_limit_bytes=63 * 1024 * 1024, dimension_semantics=("arbitrary",)
        ),
        cost_estimate=pl.CostEstimate(
            flops=2 * rows * width * cols, bytes_accessed=20 * 1024 * 1024, transcendentals=0
        ),
        name="product",
    )(*args)


def body(hidden, out_grad, route_weight, expert_ids):
    micros, tokens, choices, width = hidden.shape
    model = out_grad.shape[2]
    nx, ny = lax.axis_size("rep_0"), lax.axis_size("rep_1")
    owners = lax.axis_size(EP)
    all_tokens = micros * tokens
    per_owner = micros * CAP

    offsets = [o for pair in CHUNKS for o in pair]
    ids_row = expert_ids.reshape(1, all_tokens * choices)
    ids_by_choice = jnp.transpose(expert_ids, (2, 0, 1)).reshape(choices, all_tokens)
    weight_by_choice = jnp.transpose(route_weight, (2, 0, 1)).reshape(choices, all_tokens)

    sent_hidden = place_hidden(ids_row, hidden.reshape(all_tokens * choices, width), owners, micros)
    mine = lax.all_to_all(sent_hidden, EP, split_axis=0, concat_axis=0, tiled=True)
    mine = mine.reshape(owners * per_owner, width + LANES)

    packed = pack_columns(out_grad.reshape(all_tokens, model), ids_by_choice, weight_by_choice, offsets, micros)
    came = {}
    for (a, b), block in zip(offsets, packed):
        if (a, b) != (0, 0):
            perm = [
                (x * ny + y, ((x + a) % nx) * ny + (y + b) % ny) for x in range(nx) for y in range(ny)
            ]
            block = lax.ppermute(block, REP, perm)
        came[a, b] = block
    ring = lambda n, d: [(i, (i + d) % n) for i in range(n)]
    half = owners * per_owner // 2

    def gathered(block):
        up = lax.ppermute(block, "rep_1", ring(ny, 1))
        down = lax.ppermute(block, "rep_1", ring(ny, -1))
        top = lax.ppermute(up[:half], "rep_1", ring(ny, 1))
        bottom = lax.ppermute(down[half:], "rep_1", ring(ny, -1))
        return [block, up, down, top, bottom]

    sizes = tuple(lax.axis_size(axis) for axis in EP)
    nz = sizes[1]
    up = lambda x: lax.ppermute(x, "ep_1", ring(nz, 1))
    down = lambda x: lax.ppermute(x, "ep_1", ring(nz, -1))

    def across(arrays):
        out = [arrays[0]]
        for array, (dx, dc) in zip(arrays[1:], RELATIVE[1:]):
            perm = [
                (x * sizes[2] + c, (x + dx) % sizes[0] * sizes[2] + (c + dc) % sizes[2])
                for x in range(sizes[0])
                for c in range(sizes[2])
            ]
            out.append(lax.ppermute(array, (EP[0], EP[2]), perm))
        return out

    tie = lax.optimization_barrier

    def travelled(own):
        below, above = up(own), down(own)
        below2, above2 = up(below), down(above)
        near = place_near(sizes, own, below, above, all_tokens, per_owner)
        below2, above2, *near = tie((below2, above2, *near))
        near = across(near)
        *middle, go_up, go_down = place_middle(sizes, below2, above2, all_tokens, per_owner)
        middle = across(middle)
        below3, above3 = up(go_up), down(go_down)
        below3, above3, *near = tie((below3, above3, *near))
        *far, go_up, go_down = place_far(sizes, below3, above3, all_tokens, per_owner)
        below4, above4 = up(go_up), down(go_down)
        below4, above4, *middle = tie((below4, above4, *middle))
        final = place_last(below4, above4, per_owner)
        return [near, middle, across(far), across(final)]

    own = [assemble([came[o] for o in side]) for side in CHUNKS]
    own[0], mine = tie((own[0], mine))
    other = lax.ppermute(mine, "rep_0", ring(nx, 1))
    total = loads = None
    for n, block in enumerate((mine, other)):
        groups = travelled(own[n])
        block, from_below, from_above, top, bottom = gathered(block)
        pieces = [(block, 0, 0), (from_below, 1, 0), (from_above, 2, 0), (top, 3, 0), (bottom, 3, half)]
        total, loads = product(sizes, pieces, groups, per_owner, total, loads, n == len(CHUNKS) - 1)

    experts = owners
    expert_load = loads[0, :experts] * (experts / float(micros * tokens * nx * ny * owners * choices))
    return total[None], expert_load


def solution(mesh):
    finer = Mesh(mesh.devices.reshape(2, 4, 2, 8, 2), REP_EP)
    placed = (
        P(None, REP_EP, None, None),
        P(None, REP_EP, None),
        P(None, REP_EP, None),
        P(None, REP_EP, None),
    )
    return jax.shard_map(
        body, mesh=finer, in_specs=placed, out_specs=(P(EP, None, REP), P()), check_vma=False
    )
```

```python
import jax
import jax.numpy as jnp
from jax import lax
from jax.experimental import pallas as pl
from jax.experimental.pallas import tpu as pltpu
from jax.sharding import Mesh
from jax.sharding import PartitionSpec as P

REP = ("rep_0", "rep_1")
EP = ("ep_0", "ep_1", "ep_2")
REP_EP = REP + EP
LANES = 128
CAP = 4
META = 16
BLOCKS = 4
RELATIVE = ((0, 0), (0, 1), (1, 0), (1, 1))

STEPS = (0, 1, 3, 2)


def tn_dot(a, b):
    return lax.dot_general(a, b, (((0,), (0,)), ((), ())), preferred_element_type=jnp.float32)


def pack_columns(out_grad, ids, weight, micros):
    tokens, width = out_grad.shape
    nx, ny = lax.axis_size("rep_0"), lax.axis_size("rep_1")
    cols = width // (nx * ny)
    block = tokens // micros
    size = tokens + META

    def kernel(x_ref, ids_ref, weight_ref, *outs):
        rows = [ids_ref[k : k + 1, :].astype(jnp.float32) for k in range(2)]
        columns = [jnp.transpose(jnp.broadcast_to(row, (tokens, tokens))) for row in rows]
        there = lax.broadcasted_iota(jnp.int32, (tokens, tokens), 0)
        here = lax.broadcasted_iota(jnp.int32, (tokens, tokens), 1)
        before = (there < here) & (there // block == here // block)
        base = (lax.broadcasted_iota(jnp.int32, (1, tokens), 1) // block * CAP).astype(jnp.float32)
        line = lax.broadcasted_iota(jnp.int32, (META, tokens), 0)
        meta = jnp.zeros((META, tokens), jnp.float32)
        for k in range(2):
            hits = jnp.where(before & (columns[0] == rows[k]), 1.0, 0.0)
            hits = hits + jnp.where(before & (columns[1] == rows[k]), 1.0, 0.0)
            sub = jnp.sum(hits, axis=0, keepdims=True) + base
            value = weight_ref[k : k + 1, :]
            high = value.astype(jnp.bfloat16).astype(jnp.float32)
            middle = (value - high).astype(jnp.bfloat16).astype(jnp.float32)
            low = value - high - middle
            for at, item in enumerate((rows[k], sub, high, middle, low)):
                meta = jnp.where(line == 5 * k + at, item, meta)
        packed = meta.astype(jnp.bfloat16)
        me_x, me_y = lax.axis_index("rep_0"), lax.axis_index("rep_1")
        blank = jnp.zeros((META, cols - tokens), jnp.bfloat16)
        for out, step in zip(outs, STEPS):
            for a in range(nx):
                at = lax.rem(me_x + a, nx) * ny + lax.rem(me_y + step, ny)
                start = pl.multiple_of(at * cols, LANES)
                out[a * size : a * size + tokens, :] = x_ref[:, pl.ds(start, cols)]
                out[a * size + tokens : (a + 1) * size, :tokens] = packed
                out[a * size + tokens : (a + 1) * size, tokens:] = blank

    return pl.pallas_call(
        kernel,
        out_shape=[jax.ShapeDtypeStruct((nx * size, cols), jnp.bfloat16)] * ny,
        compiler_params=pltpu.CompilerParams(vmem_limit_bytes=24 * 1024 * 1024),
        cost_estimate=pl.CostEstimate(flops=1 << 29, bytes_accessed=4 * 1024 * 1024, transcendentals=0),
        name="pack_columns",
    )(out_grad, ids, weight)


def assemble(blocks):
    count = len(blocks)
    rows, cols = blocks[0].shape
    size = rows // 2
    tokens = size - META

    def kernel(*refs):
        for a, out_ref in enumerate(refs[count:]):
            for j in range(count):
                first = a * size
                out_ref[j * tokens : (j + 1) * tokens, :] = refs[j][first : first + tokens, :]
                data = refs[j][first + tokens : first + size, :tokens]
                out_ref[count * tokens :, j * tokens : (j + 1) * tokens] = data
            out_ref[count * tokens :, count * tokens :] = jnp.zeros((META, cols - count * tokens), jnp.bfloat16)

    return pl.pallas_call(
        kernel,
        out_shape=[jax.ShapeDtypeStruct((count * tokens + META, cols), jnp.bfloat16)] * 2,
        compiler_params=pltpu.CompilerParams(vmem_limit_bytes=16 * 1024 * 1024),
        cost_estimate=pl.CostEstimate(flops=1 << 29, bytes_accessed=4 * 1024 * 1024, transcendentals=0),
        name="assemble",
    )(*blocks)


def place_hidden(ids, hidden, owners, micros):
    pairs, width = hidden.shape
    per_owner = micros * CAP
    steps = 4
    here = owners // steps
    block = pairs // micros

    def kernel(ids_ref, h_ref, out_ref, slot_ref, count_ref):
        @pl.when(pl.program_id(0) == 0)
        def _():
            row = ids_ref[...].astype(jnp.float32)
            mine = jnp.transpose(jnp.broadcast_to(row, (pairs, pairs)))
            mine_at = lax.broadcasted_iota(jnp.int32, (pairs, pairs), 0)
            there = lax.broadcasted_iota(jnp.int32, (pairs, pairs), 1)
            before = (there < mine_at) & (there // block == mine_at // block)
            position = jnp.sum(jnp.where(before & (row == mine), 1.0, 0.0), axis=1, keepdims=True)
            base = (lax.broadcasted_iota(jnp.int32, (pairs, LANES), 0) // block * CAP).astype(jnp.float32)
            slot_ref[...] = mine[:, :LANES] * per_owner + position + base
            lane = lax.broadcasted_iota(jnp.int32, (pairs, LANES), 1).astype(jnp.float32)
            count_ref[...] = jnp.sum(jnp.where(lane == mine[:, :LANES], 1.0, 0.0), axis=0, keepdims=True)

        at = lax.broadcasted_iota(jnp.int32, (pairs, here * per_owner), 1)
        at = (at + pl.program_id(0) * (here * per_owner)).astype(jnp.float32)
        pick = jnp.where(slot_ref[:, : here * per_owner] == at, 1.0, 0.0).astype(jnp.bfloat16)
        rows = tn_dot(pick, h_ref[...]).astype(jnp.bfloat16)
        out_ref[:, :, :width] = rows.reshape(here, per_owner, width)
        first = lax.broadcasted_iota(jnp.int32, (here * per_owner, LANES), 0) % per_owner == 0
        spare = jnp.where(first, count_ref[...], 0.0).astype(jnp.bfloat16)
        out_ref[:, :, width:] = spare.reshape(here, per_owner, LANES)

    return pl.pallas_call(
        kernel,
        out_shape=jax.ShapeDtypeStruct((owners, per_owner, width + LANES), jnp.bfloat16),
        grid=(steps,),
        in_specs=[
            pl.BlockSpec((1, pairs), lambda i: (0, 0)),
            pl.BlockSpec((pairs, width), lambda i: (0, 0)),
        ],
        out_specs=pl.BlockSpec((here, per_owner, width + LANES), lambda i: (i, 0, 0)),
        scratch_shapes=[pltpu.VMEM((pairs, LANES), jnp.float32), pltpu.VMEM((1, LANES), jnp.float32)],
        compiler_params=pltpu.CompilerParams(vmem_limit_bytes=16 * 1024 * 1024),
        cost_estimate=pl.CostEstimate(
            flops=2 * owners * per_owner * pairs * width, bytes_accessed=3 * 1024 * 1024, transcendentals=0
        ),
        name="place_hidden",
    )(ids, hidden)


class Site:
    def __init__(self, sizes):
        self.nx, self.nz, self.nc = sizes
        self.x, self.z, self.c = lax.axis_index("ep_0"), lax.axis_index("ep_1"), lax.axis_index("ep_2")

    def owner(self, rel, dz):
        x = lax.rem(self.x + rel[0], self.nx)
        z = lax.rem(self.z + dz + self.nz, self.nz)
        return (x * self.nz + z) * self.nc + lax.rem(self.c + rel[1], self.nc)


def rows_for(site, ref, block, blocks, tokens, per_owner, dz):
    spot = lax.broadcasted_iota(jnp.int32, (len(RELATIVE) * per_owner, 1), 0)
    want = spot - spot // per_owner * per_owner
    for n, rel in enumerate(RELATIVE):
        want = want + jnp.where(spot // per_owner == n, site.owner(rel, dz) * per_owner, 0)
    want = want.astype(jnp.float32)
    meta = ref[blocks * tokens : blocks * tokens + META, block * tokens : (block + 1) * tokens].astype(jnp.float32)
    weight = jnp.zeros((1, 1), jnp.float32)
    hit = None
    for k in range(2):
        at = 5 * k
        mine = meta[at : at + 1] * per_owner + meta[at + 1 : at + 2] == want
        value = (meta[at + 2 : at + 3] + meta[at + 3 : at + 4]) + meta[at + 4 : at + 5]
        weight = weight + jnp.sum(jnp.where(mine, value, 0.0), axis=1, keepdims=True)
        hit = mine if hit is None else hit | mine
    pick = jnp.where(hit, 1.0, 0.0).astype(jnp.bfloat16)
    x = ref[block * tokens : (block + 1) * tokens, :]
    picked = jnp.dot(pick, x, preferred_element_type=jnp.float32)
    return (picked * weight).astype(jnp.bfloat16)


def stage(kernel, inputs, shapes, flops):
    return pl.pallas_call(
        kernel,
        out_shape=[jax.ShapeDtypeStruct(shape, jnp.bfloat16) for shape in shapes],
        compiler_params=pltpu.CompilerParams(vmem_limit_bytes=20 * 1024 * 1024),
        cost_estimate=pl.CostEstimate(flops=flops, bytes_accessed=4 * 1024 * 1024, transcendentals=0),
    )(*inputs)


def put(outs, rows, first, per_owner):
    for n in range(len(RELATIVE)):
        outs[n][first : first + per_owner, :] = rows[n * per_owner : (n + 1) * per_owner]


def place_close(sizes, messages, tokens, per_owner):
    cols = messages[0].shape[1]
    part = BLOCKS // 2
    head = part * tokens
    wide = len(RELATIVE) * per_owner

    def kernel(*refs):
        site = Site(sizes)
        messages, outs = refs[:5], refs[5:9]
        for out, ref, dz, kept in zip(refs[9:], messages[3:], (1, -1), (0, part)):
            out[:head, :] = ref[kept * tokens : kept * tokens + head, :]
            out[head : head + META, :head] = ref[BLOCKS * tokens :, kept * tokens : kept * tokens + head]
            out[head : head + META, head:] = jnp.zeros((META, cols - head), jnp.bfloat16)
            for j in range(part):
                rows = rows_for(site, ref, part - kept + j, BLOCKS, tokens, per_owner, dz)
                out[head + META + j * wide : head + META + (j + 1) * wide, :] = rows
        for m, ref in enumerate(messages):
            for j in range(BLOCKS):
                rows = rows_for(site, ref, j, BLOCKS, tokens, per_owner, 0)
                put(outs, rows, (m * BLOCKS + j) * per_owner, per_owner)

    shapes = [(5 * BLOCKS * per_owner, cols)] * len(RELATIVE)
    shapes += [(head + META + part * wide, cols)] * 2
    return stage(kernel, messages, shapes, 1 << 30)


def pass_on(sizes, below, above, tokens, per_owner):
    cols = below.shape[1]
    part = BLOCKS // 2
    wide = len(RELATIVE) * per_owner

    def kernel(below_ref, above_ref, *outs):
        site = Site(sizes)
        for out, ref, dz in zip(outs, (below_ref, above_ref), (1, -1)):
            for j in range(part):
                out[j * wide : (j + 1) * wide, :] = rows_for(site, ref, j, part, tokens, per_owner, dz)

    return stage(kernel, (below, above), [(part * wide, cols)] * 2, 1 << 29)


def place_far(sizes, messages, tokens, per_owner):
    cols = messages[0].shape[1]
    part = BLOCKS // 2
    head = part * tokens
    wide = len(RELATIVE) * per_owner

    def kernel(below_ref, above_ref, last_ref, last_above_ref, *outs):
        site = Site(sizes)
        for m, (ref, kept) in enumerate(((below_ref, 0), (above_ref, part))):
            for j in range(part):
                rows = rows_for(site, ref, j, part, tokens, per_owner, 0)
                put(outs, rows, (m * BLOCKS + kept + j) * per_owner, per_owner)
                first = head + META + j * wide
                put(outs, ref[first : first + wide, :], (m * BLOCKS + part - kept + j) * per_owner, per_owner)
        for m, ref in enumerate((last_ref, last_above_ref)):
            for j in range(part):
                put(outs, ref[j * wide : (j + 1) * wide, :], ((4 + m) * part + j) * per_owner, per_owner)

    return stage(kernel, messages, [(3 * BLOCKS * per_owner, cols)] * len(RELATIVE), 1 << 29)


GROUPS = ((0, -1, 1, -2, 2), (-3, 3, 4))


def product(sizes, pieces, groups, per_owner, total, loads, last):
    count = len(pieces)
    wide = pieces[0][0].shape[1]
    width = wide - LANES
    flat = [x for group in groups for x in group]
    cols = flat[0].shape[1]
    owners = sizes[0] * sizes[1] * sizes[2]
    per_block = owners * per_owner
    tile = 256
    first = total is None

    def kernel(*refs):
        h = refs[:count]
        spare = refs[count : 2 * count]
        sent = refs[2 * count : 2 * count + len(flat)]
        rest = refs[2 * count + len(flat) :]
        if first:
            out_ref, load_ref, cot_ref = rest
        else:
            total_ref, seen_ref, out_ref, load_ref, cot_ref = rest

        @pl.when(pl.program_id(0) == 0)
        def _():
            site = Site(sizes)
            n = 0
            for runs in GROUPS:
                for rel in RELATIVE:
                    for m, dz in enumerate(runs):
                        owner = site.owner(rel, dz)

                        def move(block, carry, n=n, m=m, owner=owner):
                            to = pl.multiple_of(block * per_block + owner * per_owner, per_owner)
                            at = pl.multiple_of((m * BLOCKS + block) * per_owner, per_owner)
                            cot_ref[pl.ds(to, per_owner), :] = sent[n][pl.ds(at, per_owner), :]
                            return carry

                        lax.fori_loop(0, BLOCKS, move, 0)
                    n += 1
            seen = None if first else seen_ref[...]
            for n in range(count):
                part = jnp.sum(spare[n][...].astype(jnp.float32), axis=0, keepdims=True)
                seen = part if seen is None else seen + part
            load_ref[...] = seen

        acc = None
        for n, (piece, block, start) in enumerate(pieces):
            at = block * per_block + start
            part = tn_dot(h[n][...], cot_ref[at : at + piece.shape[0], :])
            acc = part if acc is None else acc + part
        if not first:
            acc = acc + total_ref[...]
        out_ref[...] = acc.astype(out_ref.dtype)

    in_specs = [pl.BlockSpec((p.shape[0], tile), lambda m: (0, m)) for p, _, _ in pieces]
    in_specs += [pl.BlockSpec((p.shape[0], LANES), lambda m: (0, width // LANES)) for p, _, _ in pieces]
    in_specs += [pl.BlockSpec(x.shape, lambda m: (0, 0)) for x in flat]
    args = [p for p, _, _ in pieces] * 2 + flat
    if not first:
        in_specs += [pl.BlockSpec((tile, cols), lambda m: (m, 0)), pl.BlockSpec((1, LANES), lambda m: (0, 0))]
        args += [total, loads]
    rows = sum(p.shape[0] for p, _, _ in pieces)
    return pl.pallas_call(
        kernel,
        out_shape=[
            jax.ShapeDtypeStruct((width, cols), jnp.bfloat16 if last else jnp.float32),
            jax.ShapeDtypeStruct((1, LANES), jnp.float32),
        ],
        grid=(width // tile,),
        in_specs=in_specs,
        out_specs=[pl.BlockSpec((tile, cols), lambda m: (m, 0)), pl.BlockSpec((1, LANES), lambda m: (0, 0))],
        scratch_shapes=[pltpu.VMEM((BLOCKS * per_block, cols), jnp.bfloat16)],
        compiler_params=pltpu.CompilerParams(
            vmem_limit_bytes=63 * 1024 * 1024, dimension_semantics=("arbitrary",)
        ),
        cost_estimate=pl.CostEstimate(
            flops=2 * rows * width * cols, bytes_accessed=20 * 1024 * 1024, transcendentals=0
        ),
        name="product",
    )(*args)


def body(hidden, out_grad, route_weight, expert_ids):
    micros, tokens, choices, width = hidden.shape
    model = out_grad.shape[2]
    nx, ny = lax.axis_size("rep_0"), lax.axis_size("rep_1")
    owners = lax.axis_size(EP)
    all_tokens = micros * tokens
    per_owner = micros * CAP

    ids_row = expert_ids.reshape(1, all_tokens * choices)
    ids_by_choice = jnp.transpose(expert_ids, (2, 0, 1)).reshape(choices, all_tokens)
    weight_by_choice = jnp.transpose(route_weight, (2, 0, 1)).reshape(choices, all_tokens)

    sent_hidden = place_hidden(ids_row, hidden.reshape(all_tokens * choices, width), owners, micros)
    mine = lax.all_to_all(sent_hidden, EP, split_axis=0, concat_axis=0, tiled=True)
    mine = mine.reshape(owners * per_owner, width + LANES)

    packed = pack_columns(out_grad.reshape(all_tokens, model), ids_by_choice, weight_by_choice, micros)

    ring = lambda n, d: [(i, (i + d) % n) for i in range(n)]
    half = owners * per_owner // 2

    def gathered(block):
        up = lax.ppermute(block, "rep_1", ring(ny, 1))
        down = lax.ppermute(block, "rep_1", ring(ny, -1))
        top = lax.ppermute(up[:half], "rep_1", ring(ny, 1))
        bottom = lax.ppermute(down[half:], "rep_1", ring(ny, -1))
        return [block, up, down, top, bottom]

    sizes = tuple(lax.axis_size(axis) for axis in EP)
    nz = sizes[1]

    def hop(below, above):
        below = lax.ppermute(below, "ep_1", ring(nz, 1))
        above = lax.ppermute(above, "ep_1", ring(nz, -1))
        return below, above

    def across(arrays):
        out = [arrays[0]]
        for array, (dx, dc) in zip(arrays[1:], RELATIVE[1:]):
            perm = [
                (x * sizes[2] + c, (x + dx) % sizes[0] * sizes[2] + (c + dc) % sizes[2])
                for x in range(sizes[0])
                for c in range(sizes[2])
            ]
            out.append(lax.ppermute(array, (EP[0], EP[2]), perm))
        return out

    tie = lax.optimization_barrier
    came = [packed[0]] + [
        lax.ppermute(x, "rep_1", ring(ny, step)) for x, step in zip(packed[1:], STEPS[1:])
    ]
    own_a, crossing = assemble(came)
    own_b = lax.ppermute(crossing, "rep_0", ring(nx, 1))
    below_a, above_a = hop(own_a, own_a)
    own_b, below_a, above_a, mine = tie((own_b, below_a, above_a, mine))
    below_b, above_b = hop(own_b, own_b)
    other = lax.ppermute(mine, "rep_0", ring(nx, 1))
    below2_a, above2_a = hop(below_a, above_a)
    below2_b, above2_b = hop(below_b, above_b)
    *close_a, going_up, going_down = place_close(
        sizes, (own_a, below_a, above_a, below2_a, above2_a), all_tokens, per_owner
    )
    close_a = across(close_a)
    below3_a, above3_a = hop(going_up, going_down)
    below2_b, above2_b, other = tie((below2_b, above2_b, other))
    *close_b, going_up, going_down = place_close(
        sizes, (own_b, below_b, above_b, below2_b, above2_b), all_tokens, per_owner
    )
    close_b = across(close_b)
    below3_b, above3_b = hop(going_up, going_down)
    going_up, going_down = pass_on(sizes, below3_a, above3_a, all_tokens, per_owner)
    below4_a, above4_a = hop(going_up, going_down)
    below3_b, above3_b, *close_a = tie((below3_b, above3_b, *close_a))
    going_up, going_down = pass_on(sizes, below3_b, above3_b, all_tokens, per_owner)
    below4_b, above4_b = hop(going_up, going_down)
    far_a = across(place_far(sizes, (below3_a, above3_a, below4_a, above4_a), all_tokens, per_owner))
    below4_b, above4_b, *close_b = tie((below4_b, above4_b, *close_b))
    far_b = across(place_far(sizes, (below3_b, above3_b, below4_b, above4_b), all_tokens, per_owner))

    total = loads = None
    for n, (block, groups) in enumerate(((mine, (close_a, far_a)), (other, (close_b, far_b)))):
        block, from_below, from_above, top, bottom = gathered(block)
        pieces = [(block, 0, 0), (from_below, 1, 0), (from_above, 2, 0), (top, 3, 0), (bottom, 3, half)]
        total, loads = product(sizes, pieces, groups, per_owner, total, loads, n == 1)

    experts = owners
    expert_load = loads[0, :experts] * (experts / float(micros * tokens * nx * ny * owners * choices))
    return total[None], expert_load


def solution(mesh):
    finer = Mesh(mesh.devices.reshape(2, 4, 2, 8, 2), REP_EP)
    placed = (
        P(None, REP_EP, None, None),
        P(None, REP_EP, None),
        P(None, REP_EP, None),
        P(None, REP_EP, None),
    )
    return jax.shard_map(body, mesh=finer, in_specs=placed, out_specs=(P(EP, None, REP), P()), check_vma=False)
```

```python
import jax
import jax.numpy as jnp
from jax import lax
from jax.experimental import pallas as pl
from jax.experimental.pallas import tpu as pltpu
from jax.sharding import Mesh
from jax.sharding import PartitionSpec as P

REP = ("rep_0", "rep_1")
EP = ("ep_0", "ep_1", "ep_2")
REP_EP = REP + EP
LANES = 128
CAP = 4
META = 16
BLOCKS = 4
RELATIVE = ((0, 0), (0, 1), (1, 0), (1, 1))

STEPS = (0, 1, 3, 2)


def tn_dot(a, b):
    return lax.dot_general(a, b, (((0,), (0,)), ((), ())), preferred_element_type=jnp.float32)


def pack_columns(out_grad, ids, weight, micros):
    tokens, width = out_grad.shape
    nx, ny = lax.axis_size("rep_0"), lax.axis_size("rep_1")
    cols = width // (nx * ny)
    block = tokens // micros
    size = tokens + META

    def kernel(x_ref, ids_ref, weight_ref, *outs):
        rows = [ids_ref[k : k + 1, :].astype(jnp.float32) for k in range(2)]
        columns = [jnp.transpose(jnp.broadcast_to(row, (tokens, tokens))) for row in rows]
        there = lax.broadcasted_iota(jnp.int32, (tokens, tokens), 0)
        here = lax.broadcasted_iota(jnp.int32, (tokens, tokens), 1)
        before = (there < here) & (there // block == here // block)
        base = (lax.broadcasted_iota(jnp.int32, (1, tokens), 1) // block * CAP).astype(jnp.float32)
        line = lax.broadcasted_iota(jnp.int32, (META, tokens), 0)
        meta = jnp.zeros((META, tokens), jnp.float32)
        for k in range(2):
            hits = jnp.where(before & (columns[0] == rows[k]), 1.0, 0.0)
            hits = hits + jnp.where(before & (columns[1] == rows[k]), 1.0, 0.0)
            sub = jnp.sum(hits, axis=0, keepdims=True) + base
            value = weight_ref[k : k + 1, :]
            high = value.astype(jnp.bfloat16).astype(jnp.float32)
            middle = (value - high).astype(jnp.bfloat16).astype(jnp.float32)
            low = value - high - middle
            for at, item in enumerate((rows[k], sub, high, middle, low)):
                meta = jnp.where(line == 5 * k + at, item, meta)
        packed = meta.astype(jnp.bfloat16)
        me_x, me_y = lax.axis_index("rep_0"), lax.axis_index("rep_1")
        blank = jnp.zeros((META, cols - tokens), jnp.bfloat16)
        for out, step in zip(outs, STEPS):
            for a in range(nx):
                at = lax.rem(me_x + a, nx) * ny + lax.rem(me_y + step, ny)
                start = pl.multiple_of(at * cols, LANES)
                out[a * size : a * size + tokens, :] = x_ref[:, pl.ds(start, cols)]
                out[a * size + tokens : (a + 1) * size, :tokens] = packed
                out[a * size + tokens : (a + 1) * size, tokens:] = blank

    return pl.pallas_call(
        kernel,
        out_shape=[jax.ShapeDtypeStruct((nx * size, cols), jnp.bfloat16)] * ny,
        compiler_params=pltpu.CompilerParams(vmem_limit_bytes=24 * 1024 * 1024),
        cost_estimate=pl.CostEstimate(flops=1 << 29, bytes_accessed=4 * 1024 * 1024, transcendentals=0),
        name="pack_columns",
    )(out_grad, ids, weight)


def assemble(blocks):
    count = len(blocks)
    rows, cols = blocks[0].shape
    size = rows // 2
    tokens = size - META

    def kernel(*refs):
        for a, out_ref in enumerate(refs[count:]):
            for j in range(count):
                first = a * size
                out_ref[j * tokens : (j + 1) * tokens, :] = refs[j][first : first + tokens, :]
                data = refs[j][first + tokens : first + size, :tokens]
                out_ref[count * tokens :, j * tokens : (j + 1) * tokens] = data
            out_ref[count * tokens :, count * tokens :] = jnp.zeros((META, cols - count * tokens), jnp.bfloat16)

    return pl.pallas_call(
        kernel,
        out_shape=[jax.ShapeDtypeStruct((count * tokens + META, cols), jnp.bfloat16)] * 2,
        compiler_params=pltpu.CompilerParams(vmem_limit_bytes=16 * 1024 * 1024),
        cost_estimate=pl.CostEstimate(flops=1 << 29, bytes_accessed=4 * 1024 * 1024, transcendentals=0),
        name="assemble",
    )(*blocks)


def place_hidden(ids, hidden, owners, micros):
    pairs, width = hidden.shape
    per_owner = micros * CAP
    steps = 4
    here = owners // steps
    block = pairs // micros

    def kernel(ids_ref, h_ref, out_ref, slot_ref, count_ref):
        @pl.when(pl.program_id(0) == 0)
        def _():
            row = ids_ref[...].astype(jnp.float32)
            mine = jnp.transpose(jnp.broadcast_to(row, (pairs, pairs)))
            mine_at = lax.broadcasted_iota(jnp.int32, (pairs, pairs), 0)
            there = lax.broadcasted_iota(jnp.int32, (pairs, pairs), 1)
            before = (there < mine_at) & (there // block == mine_at // block)
            position = jnp.sum(jnp.where(before & (row == mine), 1.0, 0.0), axis=1, keepdims=True)
            base = (lax.broadcasted_iota(jnp.int32, (pairs, LANES), 0) // block * CAP).astype(jnp.float32)
            slot_ref[...] = mine[:, :LANES] * per_owner + position + base
            lane = lax.broadcasted_iota(jnp.int32, (pairs, LANES), 1).astype(jnp.float32)
            count_ref[...] = jnp.sum(jnp.where(lane == mine[:, :LANES], 1.0, 0.0), axis=0, keepdims=True)

        at = lax.broadcasted_iota(jnp.int32, (pairs, here * per_owner), 1)
        at = (at + pl.program_id(0) * (here * per_owner)).astype(jnp.float32)
        pick = jnp.where(slot_ref[:, : here * per_owner] == at, 1.0, 0.0).astype(jnp.bfloat16)
        rows = tn_dot(pick, h_ref[...]).astype(jnp.bfloat16)
        out_ref[:, :, :width] = rows.reshape(here, per_owner, width)
        first = lax.broadcasted_iota(jnp.int32, (here * per_owner, LANES), 0) % per_owner == 0
        spare = jnp.where(first, count_ref[...], 0.0).astype(jnp.bfloat16)
        out_ref[:, :, width:] = spare.reshape(here, per_owner, LANES)

    return pl.pallas_call(
        kernel,
        out_shape=jax.ShapeDtypeStruct((owners, per_owner, width + LANES), jnp.bfloat16),
        grid=(steps,),
        in_specs=[
            pl.BlockSpec((1, pairs), lambda i: (0, 0)),
            pl.BlockSpec((pairs, width), lambda i: (0, 0)),
        ],
        out_specs=pl.BlockSpec((here, per_owner, width + LANES), lambda i: (i, 0, 0)),
        scratch_shapes=[pltpu.VMEM((pairs, LANES), jnp.float32), pltpu.VMEM((1, LANES), jnp.float32)],
        compiler_params=pltpu.CompilerParams(vmem_limit_bytes=16 * 1024 * 1024),
        cost_estimate=pl.CostEstimate(
            flops=2 * owners * per_owner * pairs * width, bytes_accessed=3 * 1024 * 1024, transcendentals=0
        ),
        name="place_hidden",
    )(ids, hidden)


class Site:
    def __init__(self, sizes):
        self.nx, self.nz, self.nc = sizes
        self.x, self.z, self.c = lax.axis_index("ep_0"), lax.axis_index("ep_1"), lax.axis_index("ep_2")

    def owner(self, rel, dz):
        x = lax.rem(self.x + rel[0], self.nx)
        z = lax.rem(self.z + dz + self.nz, self.nz)
        return (x * self.nz + z) * self.nc + lax.rem(self.c + rel[1], self.nc)


def rows_for(site, ref, block, blocks, tokens, per_owner, dz):
    spot = lax.broadcasted_iota(jnp.int32, (len(RELATIVE) * per_owner, 1), 0)
    want = spot - spot // per_owner * per_owner
    for n, rel in enumerate(RELATIVE):
        want = want + jnp.where(spot // per_owner == n, site.owner(rel, dz) * per_owner, 0)
    want = want.astype(jnp.float32)
    first = pl.multiple_of(block * tokens, tokens)
    meta = ref[blocks * tokens : blocks * tokens + META, pl.ds(first, tokens)].astype(jnp.float32)
    weight = jnp.zeros((1, 1), jnp.float32)
    hit = None
    for k in range(2):
        at = 5 * k
        mine = meta[at : at + 1] * per_owner + meta[at + 1 : at + 2] == want
        value = (meta[at + 2 : at + 3] + meta[at + 3 : at + 4]) + meta[at + 4 : at + 5]
        weight = weight + jnp.sum(jnp.where(mine, value, 0.0), axis=1, keepdims=True)
        hit = mine if hit is None else hit | mine
    pick = jnp.where(hit, 1.0, 0.0).astype(jnp.bfloat16)
    x = ref[pl.ds(first, tokens), :]
    picked = jnp.dot(pick, x, preferred_element_type=jnp.float32)
    return (picked * weight).astype(jnp.bfloat16)


def stage(kernel, inputs, shapes, flops):
    return pl.pallas_call(
        kernel,
        out_shape=[jax.ShapeDtypeStruct(shape, jnp.bfloat16) for shape in shapes],
        compiler_params=pltpu.CompilerParams(vmem_limit_bytes=20 * 1024 * 1024),
        cost_estimate=pl.CostEstimate(flops=flops, bytes_accessed=4 * 1024 * 1024, transcendentals=0),
    )(*inputs)


def put(outs, rows, run, per_owner):
    first = pl.multiple_of(run * per_owner, per_owner)
    for n in range(len(RELATIVE)):
        outs[n][pl.ds(first, per_owner), :] = rows[n * per_owner : (n + 1) * per_owner]


def each(count, step):
    lax.fori_loop(0, count, lambda j, carry: (step(j), carry)[1], 0)


def place_close(sizes, messages, tokens, per_owner):
    cols = messages[0].shape[1]
    part = BLOCKS // 2
    head = part * tokens
    wide = len(RELATIVE) * per_owner

    def kernel(*refs):
        site = Site(sizes)
        messages, outs = refs[:5], refs[5:9]
        for out, ref, dz, kept in zip(refs[9:], messages[3:], (1, -1), (0, part)):
            out[:head, :] = ref[kept * tokens : kept * tokens + head, :]
            out[head : head + META, :head] = ref[BLOCKS * tokens :, kept * tokens : kept * tokens + head]
            out[head : head + META, head:] = jnp.zeros((META, cols - head), jnp.bfloat16)

            def send(j, out=out, ref=ref, dz=dz, kept=kept):
                rows = rows_for(site, ref, part - kept + j, BLOCKS, tokens, per_owner, dz)
                out[pl.ds(pl.multiple_of(head + META + j * wide, per_owner), wide), :] = rows

            each(part, send)
        for m, ref in enumerate(messages):

            def keep(j, m=m, ref=ref):
                put(outs, rows_for(site, ref, j, BLOCKS, tokens, per_owner, 0), m * BLOCKS + j, per_owner)

            each(BLOCKS, keep)

    shapes = [(5 * BLOCKS * per_owner, cols)] * len(RELATIVE)
    shapes += [(head + META + part * wide, cols)] * 2
    return stage(kernel, messages, shapes, 1 << 30)


def pass_on(sizes, below, above, tokens, per_owner):
    cols = below.shape[1]
    part = BLOCKS // 2
    wide = len(RELATIVE) * per_owner

    def kernel(below_ref, above_ref, *outs):
        site = Site(sizes)
        for out, ref, dz in zip(outs, (below_ref, above_ref), (1, -1)):

            def send(j, out=out, ref=ref, dz=dz):
                rows = rows_for(site, ref, j, part, tokens, per_owner, dz)
                out[pl.ds(pl.multiple_of(j * wide, wide), wide), :] = rows

            each(part, send)

    return stage(kernel, (below, above), [(part * wide, cols)] * 2, 1 << 29)


def place_far(sizes, messages, tokens, per_owner):
    cols = messages[0].shape[1]
    part = BLOCKS // 2
    head = part * tokens
    wide = len(RELATIVE) * per_owner

    def kernel(below_ref, above_ref, last_ref, last_above_ref, *outs):
        site = Site(sizes)
        for m, (ref, kept) in enumerate(((below_ref, 0), (above_ref, part))):

            def keep(j, m=m, ref=ref, kept=kept):
                rows = rows_for(site, ref, j, part, tokens, per_owner, 0)
                put(outs, rows, m * BLOCKS + kept + j, per_owner)
                first = pl.multiple_of(head + META + j * wide, per_owner)
                put(outs, ref[pl.ds(first, wide), :], m * BLOCKS + part - kept + j, per_owner)

            each(part, keep)
        for m, ref in enumerate((last_ref, last_above_ref)):

            def final(j, m=m, ref=ref):
                rows = ref[pl.ds(pl.multiple_of(j * wide, wide), wide), :]
                put(outs, rows, (4 + m) * part + j, per_owner)

            each(part, final)

    return stage(kernel, messages, [(3 * BLOCKS * per_owner, cols)] * len(RELATIVE), 1 << 29)


GROUPS = ((0, -1, 1, -2, 2), (-3, 3, 4))


def product(sizes, pieces, groups, per_owner, total, loads, last):
    count = len(pieces)
    wide = pieces[0][0].shape[1]
    width = wide - LANES
    flat = [x for group in groups for x in group]
    cols = flat[0].shape[1]
    owners = sizes[0] * sizes[1] * sizes[2]
    per_block = owners * per_owner
    tile = 256
    first = total is None

    def kernel(*refs):
        h = refs[:count]
        spare = refs[count : 2 * count]
        sent = refs[2 * count : 2 * count + len(flat)]
        rest = refs[2 * count + len(flat) :]
        if first:
            out_ref, load_ref, cot_ref = rest
        else:
            total_ref, seen_ref, out_ref, load_ref, cot_ref = rest

        @pl.when(pl.program_id(0) == 0)
        def _():
            site = Site(sizes)
            n = 0
            for runs in GROUPS:
                for rel in RELATIVE:
                    for m, dz in enumerate(runs):
                        owner = site.owner(rel, dz)

                        def move(block, carry, n=n, m=m, owner=owner):
                            to = pl.multiple_of(block * per_block + owner * per_owner, per_owner)
                            at = pl.multiple_of((m * BLOCKS + block) * per_owner, per_owner)
                            cot_ref[pl.ds(to, per_owner), :] = sent[n][pl.ds(at, per_owner), :]
                            return carry

                        lax.fori_loop(0, BLOCKS, move, 0)
                    n += 1
            seen = None if first else seen_ref[...]
            for n in range(count):
                part = jnp.sum(spare[n][...].astype(jnp.float32), axis=0, keepdims=True)
                seen = part if seen is None else seen + part
            load_ref[...] = seen

        acc = None
        for n, (piece, block, start) in enumerate(pieces):
            at = block * per_block + start
            part = tn_dot(h[n][...], cot_ref[at : at + piece.shape[0], :])
            acc = part if acc is None else acc + part
        if not first:
            acc = acc + total_ref[...]
        out_ref[...] = acc.astype(out_ref.dtype)

    in_specs = [pl.BlockSpec((p.shape[0], tile), lambda m: (0, m)) for p, _, _ in pieces]
    in_specs += [pl.BlockSpec((p.shape[0], LANES), lambda m: (0, width // LANES)) for p, _, _ in pieces]
    in_specs += [pl.BlockSpec(x.shape, lambda m: (0, 0)) for x in flat]
    args = [p for p, _, _ in pieces] * 2 + flat
    if not first:
        in_specs += [pl.BlockSpec((tile, cols), lambda m: (m, 0)), pl.BlockSpec((1, LANES), lambda m: (0, 0))]
        args += [total, loads]
    rows = sum(p.shape[0] for p, _, _ in pieces)
    return pl.pallas_call(
        kernel,
        out_shape=[
            jax.ShapeDtypeStruct((width, cols), jnp.bfloat16 if last else jnp.float32),
            jax.ShapeDtypeStruct((1, LANES), jnp.float32),
        ],
        grid=(width // tile,),
        in_specs=in_specs,
        out_specs=[pl.BlockSpec((tile, cols), lambda m: (m, 0)), pl.BlockSpec((1, LANES), lambda m: (0, 0))],
        scratch_shapes=[pltpu.VMEM((BLOCKS * per_block, cols), jnp.bfloat16)],
        compiler_params=pltpu.CompilerParams(
            vmem_limit_bytes=63 * 1024 * 1024, dimension_semantics=("arbitrary",)
        ),
        cost_estimate=pl.CostEstimate(
            flops=2 * rows * width * cols, bytes_accessed=20 * 1024 * 1024, transcendentals=0
        ),
        name="product",
    )(*args)


def body(hidden, out_grad, route_weight, expert_ids):
    micros, tokens, choices, width = hidden.shape
    model = out_grad.shape[2]
    nx, ny = lax.axis_size("rep_0"), lax.axis_size("rep_1")
    owners = lax.axis_size(EP)
    all_tokens = micros * tokens
    per_owner = micros * CAP

    ids_row = expert_ids.reshape(1, all_tokens * choices)
    ids_by_choice = jnp.transpose(expert_ids, (2, 0, 1)).reshape(choices, all_tokens)
    weight_by_choice = jnp.transpose(route_weight, (2, 0, 1)).reshape(choices, all_tokens)

    sent_hidden = place_hidden(ids_row, hidden.reshape(all_tokens * choices, width), owners, micros)
    mine = lax.all_to_all(sent_hidden, EP, split_axis=0, concat_axis=0, tiled=True)
    mine = mine.reshape(owners * per_owner, width + LANES)

    packed = pack_columns(out_grad.reshape(all_tokens, model), ids_by_choice, weight_by_choice, micros)

    ring = lambda n, d: [(i, (i + d) % n) for i in range(n)]
    half = owners * per_owner // 2

    def gathered(block):
        up = lax.ppermute(block, "rep_1", ring(ny, 1))
        down = lax.ppermute(block, "rep_1", ring(ny, -1))
        top = lax.ppermute(up[:half], "rep_1", ring(ny, 1))
        bottom = lax.ppermute(down[half:], "rep_1", ring(ny, -1))
        return [block, up, down, top, bottom]

    sizes = tuple(lax.axis_size(axis) for axis in EP)
    nz = sizes[1]

    def hop(below, above):
        below = lax.ppermute(below, "ep_1", ring(nz, 1))
        above = lax.ppermute(above, "ep_1", ring(nz, -1))
        return below, above

    def across(arrays):
        out = [arrays[0]]
        for array, (dx, dc) in zip(arrays[1:], RELATIVE[1:]):
            perm = [
                (x * sizes[2] + c, (x + dx) % sizes[0] * sizes[2] + (c + dc) % sizes[2])
                for x in range(sizes[0])
                for c in range(sizes[2])
            ]
            out.append(lax.ppermute(array, (EP[0], EP[2]), perm))
        return out

    tie = lax.optimization_barrier
    came = [packed[0]] + [
        lax.ppermute(x, "rep_1", ring(ny, step)) for x, step in zip(packed[1:], STEPS[1:])
    ]
    own_a, crossing = assemble(came)
    own_b = lax.ppermute(crossing, "rep_0", ring(nx, 1))
    below_a, above_a = hop(own_a, own_a)
    below_b, above_b = hop(own_b, own_b)
    other = lax.ppermute(mine, "rep_0", ring(nx, 1))
    below2_a, above2_a = hop(below_a, above_a)
    below2_b, above2_b = hop(below_b, above_b)
    *close_a, going_up, going_down = place_close(
        sizes, (own_a, below_a, above_a, below2_a, above2_a), all_tokens, per_owner
    )
    close_a = across(close_a)
    below3_a, above3_a = hop(going_up, going_down)
    below2_b, above2_b, other = tie((below2_b, above2_b, other))
    *close_b, going_up, going_down = place_close(
        sizes, (own_b, below_b, above_b, below2_b, above2_b), all_tokens, per_owner
    )
    close_b = across(close_b)
    below3_b, above3_b = hop(going_up, going_down)
    going_up, going_down = pass_on(sizes, below3_a, above3_a, all_tokens, per_owner)
    below4_a, above4_a = hop(going_up, going_down)
    below3_b, above3_b, *close_a = tie((below3_b, above3_b, *close_a))
    going_up, going_down = pass_on(sizes, below3_b, above3_b, all_tokens, per_owner)
    below4_b, above4_b = hop(going_up, going_down)
    far_a = across(place_far(sizes, (below3_a, above3_a, below4_a, above4_a), all_tokens, per_owner))
    below4_b, above4_b, *close_b = tie((below4_b, above4_b, *close_b))
    far_b = across(place_far(sizes, (below3_b, above3_b, below4_b, above4_b), all_tokens, per_owner))

    total = loads = None
    for n, (block, groups) in enumerate(((mine, (close_a, far_a)), (other, (close_b, far_b)))):
        block, from_below, from_above, top, bottom = gathered(block)
        pieces = [(block, 0, 0), (from_below, 1, 0), (from_above, 2, 0), (top, 3, 0), (bottom, 3, half)]
        total, loads = product(sizes, pieces, groups, per_owner, total, loads, n == 1)

    experts = owners
    expert_load = loads[0, :experts] * (experts / float(micros * tokens * nx * ny * owners * choices))
    return total[None], expert_load


def solution(mesh):
    finer = Mesh(mesh.devices.reshape(2, 4, 2, 8, 2), REP_EP)
    placed = (
        P(None, REP_EP, None, None),
        P(None, REP_EP, None),
        P(None, REP_EP, None),
        P(None, REP_EP, None),
    )
    return jax.shard_map(body, mesh=finer, in_specs=placed, out_specs=(P(EP, None, REP), P()), check_vma=False)
```
